128 devices in a mesh: row: 8 (over x_hi, y), col: 16 (over x_lo, z, core).
Axes of the slice: x: 4 (x_hi: 2, x_lo: 2; x = x_hi * 2 + x_lo), y: 4, z: 4, core: 2. Of those that a mesh axis runs over, the one named last changes fastest.
Arguments:
- basis: bfloat16 [40, 524288], P(None, ('row', 'col'))
- expand: float32 [3, 8, 40], replicated, may hold values from -1 to 1
- tiles: bfloat16 [3, 24576, 128, 128], P(None, ('row', 'col')), may hold values from -0.21875 to 0.21875
- tile_rows: int32 [24576], P(('row', 'col')), may hold values from 0 to 511, as said below
- tile_cols: int32 [24576], P(('row', 'col')), may hold values from 0 to 255
Outputs:
- new_block: float32 [8, 524288], P(None, ('row', 'col'))
- coefficients: float32 [8, 40], replicated
- factor: float32 [8, 8], replicated
The draws below stay inside these ranges and needn't reach their ends.
Inputs may be any that keep to these rules, and one draw needn't show every extreme that they name: `tile_rows`: each device's 192 tiles come in 16 runs of 12; the row tiles of run k are 12 distinct values from k * 32 to (k + 1) * 32 - 1.
All inputs are finite; a program needn't handle non-finite values.
Results may differ from the reference program's by a relative error of at most 0.0054.
Values may be sent and summed in bfloat16 or wider, within the bound.
A program may use at most 64 MiB of HBM per device.

```python
import math
import jax
import jax.numpy as jnp
from jax import lax

LOC = 4096
CAP = 12
TILE = 128
KD = 40
BS = 8
TPD = 192
NTOT = 524288
N_ROW = 8
N_COL = 16


def draw_basis(key, part):
    key_noise, key_common, key_lean = jax.random.split(key, 3)
    random_part = jax.random.normal(key_noise, (KD, NTOT), jnp.float32)
    common = jax.random.normal(key_common, (NTOT,), jnp.float32)
    leaning = jax.random.uniform(key_lean, (KD,), jnp.float32, -0.7, 0.7)
    return (random_part + leaning[:, None] * common[None, :]).astype(jnp.bfloat16)


def draw_tile_rows(key, part):
    region = LOC // TILE
    runs = N_ROW * N_COL * N_COL
    subkeys = jax.random.split(jax.random.fold_in(key, 7), runs)
    chosen = jax.vmap(lambda subkey: jax.random.permutation(subkey, region))(subkeys)[:, :CAP]
    offsets = jnp.arange(runs, dtype=jnp.int32) % N_COL * region
    return (chosen.astype(jnp.int32) + offsets[:, None]).reshape(runs * CAP).astype(jnp.int32)


def with_ends(array, stream_key, smallest, high):
    extent = array.shape
    place = [jax.random.randint(jax.random.fold_in(stream_key, axis), (), 0, extent[axis]) for axis in range(len(extent))]
    array = array.at[tuple(place)].set(smallest)
    longest = extent.index(max(extent))
    place[longest] = (place[longest] + 1) % extent[longest]
    return array.at[tuple(place)].set(high)


def block_scale(key, extent, shards, least, high):
    def one(dim, blocks):
        heights = jax.random.uniform(jax.random.fold_in(jax.random.fold_in(key, 6), dim), (blocks,), jnp.float32, least / len(shards), high / len(shards))
        return jnp.repeat(jnp.exp(heights), extent[dim] // blocks).reshape((-1,) + (1,) * (len(extent) - dim - 1))

    factor_of = one(*shards[0])
    for cut in shards[1:]:
        factor_of = factor_of * one(*cut)
    return factor_of


def noise(key, shape, scale, reach, pieces=(), kind=jnp.bfloat16):
    values = jax.random.normal(key, shape, jnp.float32) * scale
    if len(pieces) > 0:
        values = block_scale(key, shape, pieces, -0.22, 0.18) * values
    return jnp.clip(values, min=-reach, max=reach).astype(kind)


def setup_inputs(seed: int = 0) -> dict:
    key_of = jax.random.split(jax.random.key(seed), 6)
    return {
        "basis": draw_basis(jax.random.fold_in(key_of[5], 71), 0),
        "expand": noise(key_of[1], (3, BS, KD), KD ** -0.5, 1.0, (), jnp.float32),
        "tiles": noise(key_of[2], (3, TPD * N_ROW * N_COL, TILE, TILE), (TPD * TILE * TILE // LOC) ** -0.5, 0.21875, ((1, 128),)),
        "tile_rows": draw_tile_rows(jax.random.fold_in(key_of[5], 71), 0),
        "tile_cols": with_ends(jax.random.randint(key_of[4], (TPD * N_ROW * N_COL,), 0, N_ROW * LOC // TILE), jax.random.fold_in(key_of[4], 1), 0, (N_ROW * LOC // TILE) - 1).astype(jnp.int32),
    }


def reference(basis, expand, tiles, tile_rows, tile_cols):
    entries = LOC * N_ROW * N_COL
    inverse_root = 1.0 / math.sqrt(entries)
    highest = lax.Precision.HIGHEST
    basis_full = basis.astype(jnp.float32)
    series = jnp.einsum('mbk,kn->mbn', expand.astype(jnp.float32), basis_full, precision=highest).astype(jnp.bfloat16)
    layout = series.reshape(3, BS, N_ROW, N_COL, LOC)
    region = LOC // TILE
    slot_count = N_COL * region

    def device(index_dev, sums_row):
        index_dev = index_dev.astype(jnp.int32)
        row_index = index_dev // N_COL
        col_index = index_dev % N_COL
        columns = lax.dynamic_index_in_dim(layout, col_index, 3, keepdims=False)
        columns = columns.reshape(3, BS, N_ROW * LOC // TILE, TILE)
        start = (index_dev * TPD).astype(jnp.int32)
        matrices = lax.dynamic_slice_in_dim(tiles, start, TPD, 1).astype(jnp.float32)
        rows_here = lax.dynamic_slice_in_dim(tile_rows, start, TPD, 0)
        cols_here = lax.dynamic_slice_in_dim(tile_cols, start, TPD, 0)
        picked = jnp.take(columns, cols_here, axis=2).astype(jnp.float32)
        products = jnp.einsum('mtij,mbtj->bti', matrices, picked, precision=highest)
        onehot = (rows_here[:, None] == jnp.arange(slot_count, dtype=jnp.int32)[None, :]).astype(jnp.float32)
        partial_value = jnp.einsum('ts,bti->bsi', onehot, products, precision=highest).reshape(BS, slot_count * TILE)
        return sums_row.at[:, row_index].add(partial_value)
    sums_row = lax.fori_loop(0, N_ROW * N_COL, device, jnp.zeros((BS, N_ROW, slot_count * TILE), jnp.float32))
    applied = sums_row.reshape(BS, entries)
    first_pass = jnp.dot(applied, basis_full.T, precision=highest) * inverse_root
    projected = applied - jnp.dot(first_pass, basis_full, precision=highest) * inverse_root
    second_pass = jnp.dot(projected, basis_full.T, precision=highest) * inverse_root
    cleaned = projected - jnp.dot(second_pass, basis_full, precision=highest) * inverse_root
    coefficients = first_pass + second_pass
    gram_block = jnp.dot(cleaned, cleaned.T, precision=highest) / entries
    factor = jnp.linalg.cholesky(gram_block)
    new_block = lax.linalg.triangular_solve(factor, cleaned, left_side=True, lower=True)
    return (new_block, coefficients, factor)
```

```python
import functools
import math

import jax
import jax.numpy as jnp
from jax import lax
from jax.experimental import pallas as pl
from jax.experimental.pallas import tpu as pltpu
from jax.sharding import Mesh
from jax.sharding import PartitionSpec as P

AXES = ("xh", "y", "xl", "z", "core")
SIZES = (2, 4, 2, 4, 2)
MESH = pl.DeviceIdType.MESH
F32, BF16 = jnp.float32, jnp.bfloat16
NT = (((1,), (1,)), ((), ()))

COLS, ROWS = 16, 8
MATS, BS, KD, TILE = 3, 8, 40, 128
REGION = 32
PER = 12
SLOTS = 16
KP = 48
STACK = 80


def split3(value):
    high = value.astype(BF16).astype(F32)
    rest = value - high
    middle = rest.astype(BF16).astype(F32)
    return high, middle, rest - middle


def step_kernel(
    basis_hbm, expand_hbm, rows_hbm, cols_hbm, tiles, st, total, pq,
    basis, expand, rows, cols, a_vm, xb, xf, acc, ysend, yrecv, rf, app, onehot, ids_s, ids_r, c1, c2, m1, m2, cw,
    in_sem, tile_sem, g_send, g_recv, i_send, i_recv, c1_send, c1_recv, c2_send, c2_recv,
    y_send, y_recv, m1_send, m1_recv, m2_send, m2_recv,
):
    xh, y, xl, z, core = (lax.axis_index(a) for a in AXES)
    row, col = xh * 4 + y, xl * 8 + z * 2 + core

    def col_peer(j):
        px, pz, pk = lax.rem(xl + j // 8, 2), lax.rem(z + (j // 2) % 4, 4), lax.rem(core + j % 2, 2)
        return (xh, y, px, pz, pk), px * 8 + pz * 2 + pk

    def col_source(j):
        px, pz, pk = lax.rem(xl + j // 8, 2), lax.rem(z + 4 - (j // 2) % 4, 4), lax.rem(core + j % 2, 2)
        return px * 8 + pz * 2 + pk

    def row_peer(j):
        ph, py = lax.rem(xh + j // 4, 2), lax.rem(y + j % 4, 4)
        return (ph, py, xl, z, core)

    def remote(src, dst, send, recv, device):
        return pltpu.make_async_remote_copy(
            src_ref=src, dst_ref=dst, send_sem=send, recv_sem=recv, device_id=device, device_id_type=MESH
        )

    barrier = pltpu.get_barrier_semaphore()
    for j in range(1, ROWS):
        pl.semaphore_signal(barrier, inc=1, device_id=row_peer(j), device_id_type=MESH)
    for j in range(1, COLS):
        pl.semaphore_signal(barrier, inc=1, device_id=col_peer(j)[0], device_id_type=MESH)

    in_copies = [
        pltpu.make_async_copy(src, dst, in_sem.at[i])
        for i, (src, dst) in enumerate(
            ((basis_hbm, basis), (expand_hbm, expand), (rows_hbm, rows), (cols_hbm, cols))
        )
    ]
    for copy in in_copies:
        copy.start()
    tile_copies = []
    for m in range(MATS):
        for q in range(4):
            part = pl.ds(48 * q, 48)
            copy = pltpu.make_async_copy(tiles.at[m, part], a_vm.at[m, part], tile_sem.at[m, q])
            copy.start()
            tile_copies.append(copy)

    in_copies[0].wait()
    in_copies[1].wait()
    coef = jnp.concatenate([expand[m] for m in range(MATS)], axis=0)
    lhs = jnp.concatenate(split3(coef), axis=0).astype(BF16)
    for n in range(8):
        wide = jnp.dot(lhs, basis[:, n * 512 : (n + 1) * 512], preferred_element_type=F32)
        for m in range(MATS):
            a, b, c = (wide[24 * i + 8 * m : 24 * i + 8 * m + 8] for i in range(3))
            value = (c + b) + a
            for h in range(2):
                pair = jnp.concatenate(
                    [value[:, (2 * h + i) * TILE : (2 * h + i + 1) * TILE] for i in range(2)], axis=0
                )
                xb[row, m, 64 * (n // 2) + 32 * (n % 2) + 16 * h : 64 * (n // 2) + 32 * (n % 2) + 16 * h + 16, :] = pair.astype(BF16)

    pl.semaphore_wait(barrier, ROWS + COLS - 2)

    up, down = lax.rem(y + 1, 4), lax.rem(y + 3, 4)
    far, other = lax.rem(y + 2, 4), 1 - xh
    to_up, to_down, to_other = (xh, up, xl, z, core), (xh, down, xl, z, core), (other, y, xl, z, core)
    whole, first, second = pl.ds(0, 256), pl.ds(0, 128), pl.ds(128, 128)

    def gather(m, i, slot, part, device):
        ref = xb.at[slot, m, part]
        return remote(ref, ref, g_send.at[m, i], g_recv.at[m, i], device)

    def moves(m):
        return (
            gather(m, 0, row, whole, to_up),
            gather(m, 1, row, whole, to_down),
            gather(m, 2, row, whole, to_other),
            gather(m, 3, xh * 4 + down, first, to_up),
            gather(m, 4, xh * 4 + up, second, to_down),
            gather(m, 5, other * 4 + y, whole, to_up),
            gather(m, 6, other * 4 + y, whole, to_down),
            gather(m, 7, xh * 4 + far, first, to_other),
            gather(m, 8, xh * 4 + far, second, to_other),
        )

    hops = [moves(m) for m in range(MATS)]
    for m in range(MATS):
        for i in (2, 0, 1):
            hops[m][i].start()

    in_copies[2].wait()
    in_copies[3].wait()

    def fill_ids(k, carry):
        for u in range(SLOTS):
            if u < PER:
                value = rows[k * PER + u] - k * REGION
            else:
                value = jnp.int32(-1)
            ids_s[k, u : u + 1, :] = jnp.full((1, TILE), value, jnp.int32)
        return carry

    lax.fori_loop(0, COLS, fill_ids, 0)
    id_copies = []
    for j in range(1, COLS):
        device, k = col_peer(j)
        copy = remote(ids_s.at[k], ids_r.at[col], i_send.at[j], i_recv.at[j], device)
        copy.start()
        id_copies.append(copy)
    ids_r[col] = ids_s[col]

    st[0:KD, :] = basis[...]
    st[KD:KP, :] = jnp.zeros((KP - KD, st.shape[1]), BF16)
    own = lax.dot_general(st[0:KP, :], st[0:KP, :], NT, preferred_element_type=F32)
    cw[...] = jnp.zeros(cw.shape, F32)
    cw[:, 0:KP] = own
    packed = cw[0:16, :] + pltpu.roll(cw[16:32, :], 40, 1) + pltpu.roll(cw[32:48, :], 80, 1)
    c1[col] = packed
    c1_copies = []
    for j in range(1, COLS):
        device, _ = col_peer(j)
        copy = remote(c1.at[col], c1.at[col], c1_send.at[j], c1_recv.at[j], device)
        copy.start()
        c1_copies.append(copy)

    def relay(m):
        h = hops[m]
        h[0].wait_recv()
        h[3].start()
        h[1].wait_recv()
        h[4].start()
        h[2].wait_recv()
        h[5].start()
        h[6].start()
        h[3].wait_recv()
        h[7].start()
        h[4].wait_recv()
        h[8].start()

    def arrive(m):
        for i in (5, 6, 7, 8):
            hops[m][i].wait_recv()
        for r in range(ROWS):
            xf[r * REGION : (r + 1) * REGION] = xb[r, m].astype(F32).reshape(REGION, BS, TILE)
        for q in range(4):
            tile_copies[4 * m + q].wait()

    zero = jnp.zeros((BS, TILE), F32)

    def pair_product(m, t):
        x0, x1 = xf[cols[t]], xf[cols[t + 1]]
        lhs = jnp.concatenate(
            [jnp.concatenate([x0, zero], axis=1), jnp.concatenate([zero, x1], axis=1)], axis=0
        ).astype(BF16)
        rhs = jnp.concatenate([a_vm[m, t], a_vm[m, t + 1]], axis=1)
        return lax.dot_general(lhs, rhs, NT, preferred_element_type=F32)

    def run_first(k, carry):
        for p in range(PER // 2):
            acc[k, 16 * p : 16 * p + 16, :] = pair_product(0, k * PER + 2 * p)
        return carry

    def run_second(k, carry):
        for p in range(PER // 2):
            acc[k, 16 * p : 16 * p + 16, :] += pair_product(1, k * PER + 2 * p)
        return carry

    def run_last(k):
        for p in range(PER // 2):
            part = slice(16 * p, 16 * p + 16)
            ysend[k, part, :] = (acc[k, part, :] + pair_product(2, k * PER + 2 * p)).astype(BF16)

    relay(0)
    relay(1)
    arrive(0)
    lax.fori_loop(0, COLS, run_first, 0)
    relay(2)

    for copy in c1_copies:
        copy.wait_recv()
    half = c1[0]
    for k in range(1, COLS):
        half = half + c1[k]
    c2[row] = half
    c2_copies = []
    for j in range(1, ROWS):
        copy = remote(c2.at[row], c2.at[row], c2_send.at[j], c2_recv.at[j], row_peer(j))
        copy.start()
        c2_copies.append(copy)

    for copy in id_copies:
        copy.wait_recv()
    lane = lax.broadcasted_iota(jnp.int32, (COLS * SLOTS, TILE), 1)
    chosen = jnp.where(ids_r[...].reshape(COLS * SLOTS, TILE) == lane, 1.0, 0.0).astype(F32)
    onehot[...] = chosen.T[0:REGION, :].astype(BF16)
    for k in range(COLS):
        rf[k, PER * BS :, :] = jnp.zeros(((SLOTS - PER) * BS, TILE), F32)

    arrive(1)
    lax.fori_loop(0, COLS, run_second, 0)

    for copy in c2_copies:
        copy.wait_recv()
    full = c2[0]
    for r in range(1, ROWS):
        full = full + c2[r]
    lanes = lax.broadcasted_iota(jnp.int32, (16, TILE), 1)
    keep = lanes < KD
    for i in range(3):
        cw[16 * i : 16 * i + 16, :] = jnp.where(keep, full if i == 0 else pltpu.roll(full, TILE - 40 * i, 1), 0.0)
    entries = float(st.shape[1] * ROWS * COLS)
    corr = cw[:, 0:KP] * (1.0 / entries)
    eye = jnp.where(
        lax.broadcasted_iota(jnp.int32, (KP, KP), 0) == lax.broadcasted_iota(jnp.int32, (KP, KP), 1), 1.0, 0.0
    ).astype(F32)
    dot = functools.partial(jnp.dot, precision=lax.Precision.HIGHEST, preferred_element_type=F32)
    corr2 = dot(corr, corr)
    pq[0] = 2.0 * eye - corr
    pq[1] = 4.0 * eye - 6.0 * corr + 4.0 * corr2 - dot(corr2, corr)

    arrive(2)

    def result_copy(j):
        device, k = col_peer(j)
        return remote(ysend.at[k], yrecv.at[col], y_send.at[j], y_recv.at[j], device)

    def last(j, carry):
        run_last(col_peer(j)[1])
        result_copy(j).start()
        return carry

    lax.fori_loop(1, COLS, last, 0)
    run_last(col)
    rf[col, 0 : PER * BS, :] = ysend[col].astype(F32)

    def landed(j, carry):
        k = col_source(j)
        result_copy(j).wait_recv()
        rf[k, 0 : PER * BS, :] = yrecv[k].astype(F32)
        return carry

    lax.fori_loop(1, COLS, landed, 0)

    for b in range(0, BS, 2):
        pair = [
            jnp.concatenate([rf[k, pl.ds(b + i, SLOTS, stride=BS), :] for k in range(COLS)], axis=0) for i in range(2)
        ]
        both = jnp.dot(onehot[...], jnp.concatenate(pair, axis=1).astype(BF16), preferred_element_type=F32)
        for i in range(2):
            app[pl.ds(b + i, REGION, stride=BS), :] = both[:, i * TILE : (i + 1) * TILE]
    for s in range(REGION):
        parts = split3(app[s * BS : (s + 1) * BS, :])
        st[KP:STACK, s * TILE : (s + 1) * TILE] = jnp.concatenate([*parts, zero], axis=0).astype(BF16)

    inner = lax.dot_general(st[KP:STACK, :], st[...], NT, preferred_element_type=F32)
    m1[col, :, 0:STACK] = (inner[16:24] + inner[8:16]) + inner[0:8]
    m1[col, :, STACK:] = jnp.zeros((BS, TILE - STACK), F32)
    m1_copies = []
    for j in range(1, COLS):
        device, _ = col_peer(j)
        copy = remote(m1.at[col], m1.at[col], m1_send.at[j], m1_recv.at[j], device)
        copy.start()
        m1_copies.append(copy)
    for copy in m1_copies:
        copy.wait_recv()
    half = m1[0]
    for k in range(1, COLS):
        half = half + m1[k]
    m2[row] = half
    m2_copies = []
    for j in range(1, ROWS):
        copy = remote(m2.at[row], m2.at[row], m2_send.at[j], m2_recv.at[j], row_peer(j))
        copy.start()
        m2_copies.append(copy)
    for copy in m2_copies:
        copy.wait_recv()
    full = m2[0]
    for r in range(1, ROWS):
        full = full + m2[r]
    total[...] = full

    for m in range(MATS):
        for copy in hops[m]:
            copy.wait_send()
    for copy in (*id_copies, *c1_copies, *c2_copies, *m1_copies, *m2_copies):
        copy.wait_send()

    def sent(j, carry):
        result_copy(j).wait_send()
        return carry

    lax.fori_loop(1, COLS, sent, 0)


def final_kernel(st, total, pq, new_block, coefficients, factor, *, entries):
    inverse_root = 1.0 / math.sqrt(entries)
    dot = functools.partial(lax.dot_general, precision=lax.Precision.HIGHEST, preferred_element_type=F32)
    nn = (((1,), (0,)), ((), ()))
    tot = total[...]
    raw = tot[:, 0:KP] * inverse_root
    energy = (
        pltpu.roll(tot, TILE - KP, 1) + pltpu.roll(tot, TILE - KP - 8, 1) + pltpu.roll(tot, TILE - KP - 16, 1)
    )[:, 0:BS]
    coef = dot(raw, pq[0], nn)
    gram = (energy - dot(dot(raw, pq[1], nn), raw, NT)) * (1.0 / entries)
    coefficients[...] = coef[:, 0:KD]

    sub = lax.broadcasted_iota(jnp.int32, (BS, TILE), 0)
    lane = lax.broadcasted_iota(jnp.int32, (BS, TILE), 1)
    unit = (lane == sub + KP) | (lane == sub + KP + 8) | (lane == sub + KP + 16)
    target = jnp.where(unit, 1.0, 0.0).astype(F32)
    target = target + jnp.concatenate([coef * -inverse_root, jnp.zeros((BS, TILE - KP), F32)], axis=1)
    left = jnp.concatenate([gram, jnp.zeros((BS, TILE - BS), F32)], axis=1)
    lower = jnp.zeros((BS, TILE), F32)
    for j in range(BS):
        root = jnp.sqrt(left[j : j + 1, j : j + 1])
        scale = jnp.broadcast_to(1.0 / root, (BS, 1))
        column = jnp.broadcast_to(left[:, j : j + 1] * scale, (BS, TILE))
        below = jnp.where(sub > j, column, 0.0)
        lower = jnp.where((lane == j) & (sub >= j), column, lower)
        solved = jnp.broadcast_to(target[j : j + 1, :], (BS, TILE)) * scale
        target = jnp.where(sub == j, solved, target - below * solved)
        left = left - below * (jnp.broadcast_to(left[j : j + 1, :], (BS, TILE)) * scale)
    factor[...] = lower[:, 0:BS]
    mix = jnp.concatenate(split3(target[:, 0:STACK]), axis=0).astype(BF16)
    length = st.shape[1]
    for n in range(length // 512):
        part = slice(n * 512, (n + 1) * 512)
        wide = jnp.dot(mix, st[:, part], preferred_element_type=F32)
        new_block[:, part] = (wide[16:24] + wide[8:16]) + wide[0:8]


def shards(basis, expand, tiles, tile_rows, tile_cols):
    length = basis.shape[1]
    vmem = pl.BlockSpec(memory_space=pltpu.VMEM)
    hbm = pl.BlockSpec(memory_space=pltpu.HBM)
    dma = pltpu.SemaphoreType.DMA
    st, total, pq = pl.pallas_call(
        step_kernel,
        out_shape=(
            jax.ShapeDtypeStruct((STACK, length), BF16),
            jax.ShapeDtypeStruct((BS, TILE), F32),
            jax.ShapeDtypeStruct((2, KP, KP), F32),
        ),
        in_specs=[hbm] * 5,
        out_specs=(vmem, vmem, vmem),
        scratch_shapes=[
            pltpu.VMEM(basis.shape, BF16),
            pltpu.VMEM(expand.shape, F32),
            pltpu.SMEM(tile_rows.shape, jnp.int32),
            pltpu.SMEM(tile_cols.shape, jnp.int32),
            pltpu.VMEM(tiles.shape, BF16),
            pltpu.VMEM((ROWS, MATS, 256, TILE), BF16),
            pltpu.VMEM((ROWS * REGION, BS, TILE), F32),
            pltpu.VMEM((COLS, PER * BS, TILE), F32),
            pltpu.VMEM((COLS, PER * BS, TILE), BF16),
            pltpu.VMEM((COLS, PER * BS, TILE), BF16),
            pltpu.VMEM((COLS, SLOTS * BS, TILE), F32),
            pltpu.VMEM((REGION * BS, TILE), F32),
            pltpu.VMEM((REGION, COLS * SLOTS), BF16),
            pltpu.VMEM((COLS, SLOTS, TILE), jnp.int32),
            pltpu.VMEM((COLS, SLOTS, TILE), jnp.int32),
            pltpu.VMEM((COLS, 16, TILE), F32),
            pltpu.VMEM((ROWS, 16, TILE), F32),
            pltpu.VMEM((COLS, BS, TILE), F32),
            pltpu.VMEM((ROWS, BS, TILE), F32),
            pltpu.VMEM((KP, TILE), F32),
            dma((4,)),
            dma((MATS, 4)),
            dma((MATS, 9)), dma((MATS, 9)),
            dma((COLS,)), dma((COLS,)),
            dma((COLS,)), dma((COLS,)),
            dma((ROWS,)), dma((ROWS,)),
            dma((COLS,)), dma((COLS,)),
            dma((COLS,)), dma((COLS,)),
            dma((ROWS,)), dma((ROWS,)),
        ],
        compiler_params=pltpu.CompilerParams(
            collective_id=0, has_side_effects=True, vmem_limit_bytes=36 * 2**20
        ),
        name="toar_step",
    )(basis, expand, tile_rows, tile_cols, tiles)
    return tuple(
        pl.pallas_call(
            functools.partial(final_kernel, entries=length * ROWS * COLS),
            out_shape=(
                jax.ShapeDtypeStruct((BS, length), F32),
                jax.ShapeDtypeStruct((BS, KD), F32),
                jax.ShapeDtypeStruct((BS, BS), F32),
            ),
            in_specs=[vmem, vmem, vmem],
            out_specs=(vmem, vmem, vmem),
            compiler_params=pltpu.CompilerParams(vmem_limit_bytes=8 * 2**20),
            name="toar_final",
        )(st, total, pq)
    )


def solution(mesh):
    finer = Mesh(mesh.devices.reshape(SIZES), AXES)
    return jax.shard_map(
        shards,
        mesh=finer,
        in_specs=(P(None, AXES), P(), P(None, AXES, None, None), P(AXES), P(AXES)),
        out_specs=(P(None, AXES), P(), P()),
        check_vma=False,
    )
```

```python
import functools
import math

import jax
import jax.numpy as jnp
from jax import lax
from jax.experimental import pallas as pl
from jax.experimental.pallas import tpu as pltpu
from jax.sharding import Mesh
from jax.sharding import PartitionSpec as P

AXES = ("xh", "y", "xl", "z", "core")
SIZES = (2, 4, 2, 4, 2)
MESH = pl.DeviceIdType.MESH
F32, BF16 = jnp.float32, jnp.bfloat16
NT = (((1,), (1,)), ((), ()))

COLS, ROWS = 16, 8
MATS, BS, KD, TILE = 3, 8, 40, 128
REGION = 32
PER = 12
SLOTS = 16
KP = 48
STACK = 80


def split3(value):
    high = value.astype(BF16).astype(F32)
    rest = value - high
    middle = rest.astype(BF16).astype(F32)
    return high, middle, rest - middle


def step_kernel(
    basis_hbm, expand_hbm, rows_hbm, cols_hbm, tiles, st, total, pq,
    basis, expand, rows, cols, a_vm, xb, xf, acc, ysend, yrecv, rf, app, onehot, ids_s, ids_r, c1, c2, m1, m2, cw,
    in_sem, tile_sem, g_send, g_recv, i_send, i_recv, c1_send, c1_recv, c2_send, c2_recv,
    y_send, y_recv, m1_send, m1_recv, m2_send, m2_recv,
):
    xh, y, xl, z, core = (lax.axis_index(a) for a in AXES)
    row, col = xh * 4 + y, xl * 8 + z * 2 + core

    def col_peer(j):
        px, pz, pk = lax.rem(xl + j // 8, 2), lax.rem(z + (j // 2) % 4, 4), lax.rem(core + j % 2, 2)
        return (xh, y, px, pz, pk), px * 8 + pz * 2 + pk

    def col_source(j):
        px, pz, pk = lax.rem(xl + j // 8, 2), lax.rem(z + 4 - (j // 2) % 4, 4), lax.rem(core + j % 2, 2)
        return px * 8 + pz * 2 + pk

    def row_peer(j):
        ph, py = lax.rem(xh + j // 4, 2), lax.rem(y + j % 4, 4)
        return (ph, py, xl, z, core)

    def remote(src, dst, send, recv, device):
        return pltpu.make_async_remote_copy(
            src_ref=src, dst_ref=dst, send_sem=send, recv_sem=recv, device_id=device, device_id_type=MESH
        )

    barrier = pltpu.get_barrier_semaphore()
    for j in range(1, ROWS):
        pl.semaphore_signal(barrier, inc=1, device_id=row_peer(j), device_id_type=MESH)
    for j in range(1, COLS):
        pl.semaphore_signal(barrier, inc=1, device_id=col_peer(j)[0], device_id_type=MESH)

    in_copies = [
        pltpu.make_async_copy(src, dst, in_sem.at[i])
        for i, (src, dst) in enumerate(
            ((basis_hbm, basis), (expand_hbm, expand), (rows_hbm, rows), (cols_hbm, cols))
        )
    ]
    for copy in in_copies:
        copy.start()
    in_copies[0].wait()
    in_copies[1].wait()
    tile_copies = []
    for m in range(MATS):
        for q in range(4):
            part = pl.ds(48 * q, 48)
            copy = pltpu.make_async_copy(tiles.at[m, part], a_vm.at[m, part], tile_sem.at[m, q])
            copy.start()
            tile_copies.append(copy)

    coef = jnp.concatenate([expand[m] for m in range(MATS)], axis=0)
    lhs = jnp.concatenate(split3(coef), axis=0).astype(BF16)
    for n in range(8):
        wide = jnp.dot(lhs, basis[:, n * 512 : (n + 1) * 512], preferred_element_type=F32)
        for m in range(MATS):
            a, b, c = (wide[24 * i + 8 * m : 24 * i + 8 * m + 8] for i in range(3))
            value = (c + b) + a
            for h in range(2):
                pair = jnp.concatenate(
                    [value[:, (2 * h + i) * TILE : (2 * h + i + 1) * TILE] for i in range(2)], axis=0
                )
                xb[row, m, 64 * (n // 2) + 32 * (n % 2) + 16 * h : 64 * (n // 2) + 32 * (n % 2) + 16 * h + 16, :] = pair.astype(BF16)

    pl.semaphore_wait(barrier, ROWS + COLS - 2)

    up, down = lax.rem(y + 1, 4), lax.rem(y + 3, 4)
    far, other = lax.rem(y + 2, 4), 1 - xh
    to_up, to_down, to_other = (xh, up, xl, z, core), (xh, down, xl, z, core), (other, y, xl, z, core)
    whole, first, second = pl.ds(0, 256), pl.ds(0, 128), pl.ds(128, 128)

    def gather(m, i, slot, part, device):
        ref = xb.at[slot, m, part]
        return remote(ref, ref, g_send.at[m, i], g_recv.at[m, i], device)

    def moves(m):
        return (
            gather(m, 0, row, whole, to_up),
            gather(m, 1, row, whole, to_down),
            gather(m, 2, row, whole, to_other),
            gather(m, 3, xh * 4 + down, first, to_up),
            gather(m, 4, xh * 4 + up, second, to_down),
            gather(m, 5, other * 4 + y, whole, to_up),
            gather(m, 6, other * 4 + y, whole, to_down),
            gather(m, 7, xh * 4 + far, first, to_other),
            gather(m, 8, xh * 4 + far, second, to_other),
        )

    hops = [moves(m) for m in range(MATS)]
    for m in range(MATS):
        for i in (2, 0, 1):
            hops[m][i].start()

    in_copies[2].wait()
    in_copies[3].wait()

    def fill_ids(k, carry):
        for u in range(SLOTS):
            if u < PER:
                value = rows[k * PER + u] - k * REGION
            else:
                value = jnp.int32(-1)
            ids_s[k, u : u + 1, :] = jnp.full((1, TILE), value, jnp.int32)
        return carry

    lax.fori_loop(0, COLS, fill_ids, 0)
    id_copies = []
    for j in range(1, COLS):
        device, k = col_peer(j)
        copy = remote(ids_s.at[k], ids_r.at[col], i_send.at[j], i_recv.at[j], device)
        copy.start()
        id_copies.append(copy)
    ids_r[col] = ids_s[col]

    st[0:KD, :] = basis[...]
    st[KD:KP, :] = jnp.zeros((KP - KD, st.shape[1]), BF16)
    own = lax.dot_general(st[0:KP, :], st[0:KP, :], NT, preferred_element_type=F32)
    cw[...] = jnp.zeros(cw.shape, F32)
    cw[:, 0:KP] = own
    packed = cw[0:16, :] + pltpu.roll(cw[16:32, :], 40, 1) + pltpu.roll(cw[32:48, :], 80, 1)
    c1[col] = packed
    c1_copies = []
    for j in range(1, COLS):
        device, _ = col_peer(j)
        copy = remote(c1.at[col], c1.at[col], c1_send.at[j], c1_recv.at[j], device)
        copy.start()
        c1_copies.append(copy)

    def arrive(m):
        for i in (5, 6, 7, 8):
            hops[m][i].wait_recv()
        for r in range(ROWS):
            xf[r * REGION : (r + 1) * REGION] = xb[r, m].astype(F32).reshape(REGION, BS, TILE)
        for q in range(4):
            tile_copies[4 * m + q].wait()

    zero = jnp.zeros((BS, TILE), F32)

    def pair_product(m, t):
        x0, x1 = xf[cols[t]], xf[cols[t + 1]]
        lhs = jnp.concatenate(
            [jnp.concatenate([x0, zero], axis=1), jnp.concatenate([zero, x1], axis=1)], axis=0
        ).astype(BF16)
        rhs = jnp.concatenate([a_vm[m, t], a_vm[m, t + 1]], axis=1)
        return lax.dot_general(lhs, rhs, NT, preferred_element_type=F32)

    def run_first(k, carry):
        for p in range(PER // 2):
            acc[k, 16 * p : 16 * p + 16, :] = pair_product(0, k * PER + 2 * p)
        return carry

    def run_second(k, carry):
        for p in range(PER // 2):
            acc[k, 16 * p : 16 * p + 16, :] += pair_product(1, k * PER + 2 * p)
        return carry

    def run_last(k):
        for p in range(PER // 2):
            part = slice(16 * p, 16 * p + 16)
            ysend[k, part, :] = (acc[k, part, :] + pair_product(2, k * PER + 2 * p)).astype(BF16)

    for h in hops:
        h[0].wait_recv()
        h[3].start()
        h[1].wait_recv()
        h[4].start()
    for h in hops:
        h[2].wait_recv()
        h[5].start()
        h[6].start()
    for h in hops:
        h[3].wait_recv()
        h[7].start()
        h[4].wait_recv()
        h[8].start()

    for copy in id_copies:
        copy.wait_recv()
    lane = lax.broadcasted_iota(jnp.int32, (COLS * SLOTS, TILE), 1)
    chosen = jnp.where(ids_r[...].reshape(COLS * SLOTS, TILE) == lane, 1.0, 0.0).astype(F32)
    onehot[...] = chosen.T[0:REGION, :].astype(BF16)
    for k in range(COLS):
        rf[k, PER * BS :, :] = jnp.zeros(((SLOTS - PER) * BS, TILE), F32)

    arrive(0)
    lax.fori_loop(0, COLS, run_first, 0, unroll=COLS)
    arrive(1)
    lax.fori_loop(0, COLS, run_second, 0, unroll=COLS)

    arrive(2)

    def result_copy(j):
        device, k = col_peer(j)
        return remote(ysend.at[k], yrecv.at[col], y_send.at[j], y_recv.at[j], device)

    def last(j, carry):
        run_last(col_peer(j)[1])
        result_copy(j).start()
        return carry

    lax.fori_loop(1, COLS, last, 0, unroll=COLS - 1)
    run_last(col)

    for copy in c1_copies:
        copy.wait_recv()
    half = c1[0]
    for k in range(1, COLS):
        half = half + c1[k]
    c2[row] = half
    c2_copies = []
    for j in range(1, ROWS):
        copy = remote(c2.at[row], c2.at[row], c2_send.at[j], c2_recv.at[j], row_peer(j))
        copy.start()
        c2_copies.append(copy)

    rf[col, 0 : PER * BS, :] = ysend[col].astype(F32)

    def landed(j, carry):
        k = col_source(j)
        result_copy(j).wait_recv()
        rf[k, 0 : PER * BS, :] = yrecv[k].astype(F32)
        return carry

    lax.fori_loop(1, COLS, landed, 0, unroll=COLS - 1)

    for b in range(0, BS, 2):
        pair = [
            jnp.concatenate([rf[k, pl.ds(b + i, SLOTS, stride=BS), :] for k in range(COLS)], axis=0) for i in range(2)
        ]
        both = jnp.dot(onehot[...], jnp.concatenate(pair, axis=1).astype(BF16), preferred_element_type=F32)
        for i in range(2):
            app[pl.ds(b + i, REGION, stride=BS), :] = both[:, i * TILE : (i + 1) * TILE]
    for s in range(REGION):
        parts = split3(app[s * BS : (s + 1) * BS, :])
        st[KP:STACK, s * TILE : (s + 1) * TILE] = jnp.concatenate([*parts, zero], axis=0).astype(BF16)

    inner = lax.dot_general(st[KP:STACK, :], st[...], NT, preferred_element_type=F32)
    m1[col, :, 0:STACK] = (inner[16:24] + inner[8:16]) + inner[0:8]
    m1[col, :, STACK:] = jnp.zeros((BS, TILE - STACK), F32)
    m1_copies = []
    for j in range(1, COLS):
        device, _ = col_peer(j)
        copy = remote(m1.at[col], m1.at[col], m1_send.at[j], m1_recv.at[j], device)
        copy.start()
        m1_copies.append(copy)
    for copy in c2_copies:
        copy.wait_recv()
    full = c2[0]
    for r in range(1, ROWS):
        full = full + c2[r]
    lanes = lax.broadcasted_iota(jnp.int32, (16, TILE), 1)
    keep = lanes < KD
    for i in range(3):
        cw[16 * i : 16 * i + 16, :] = jnp.where(keep, full if i == 0 else pltpu.roll(full, TILE - 40 * i, 1), 0.0)
    entries = float(st.shape[1] * ROWS * COLS)
    corr = cw[:, 0:KP] * (1.0 / entries)
    eye = jnp.where(
        lax.broadcasted_iota(jnp.int32, (KP, KP), 0) == lax.broadcasted_iota(jnp.int32, (KP, KP), 1), 1.0, 0.0
    ).astype(F32)
    dot = functools.partial(jnp.dot, precision=lax.Precision.HIGHEST, preferred_element_type=F32)
    corr2 = dot(corr, corr)
    pq[0] = 2.0 * eye - corr
    pq[1] = 4.0 * eye - 6.0 * corr + 4.0 * corr2 - dot(corr2, corr)

    for copy in m1_copies:
        copy.wait_recv()
    half = m1[0]
    for k in range(1, COLS):
        half = half + m1[k]
    m2[row] = half
    m2_copies = []
    for j in range(1, ROWS):
        copy = remote(m2.at[row], m2.at[row], m2_send.at[j], m2_recv.at[j], row_peer(j))
        copy.start()
        m2_copies.append(copy)
    for copy in m2_copies:
        copy.wait_recv()
    full = m2[0]
    for r in range(1, ROWS):
        full = full + m2[r]
    total[...] = full

    for m in range(MATS):
        for copy in hops[m]:
            copy.wait_send()
    for copy in (*id_copies, *c1_copies, *c2_copies, *m1_copies, *m2_copies):
        copy.wait_send()

    def sent(j, carry):
        result_copy(j).wait_send()
        return carry

    lax.fori_loop(1, COLS, sent, 0)


def final_kernel(st, total, pq, new_block, coefficients, factor, *, entries):
    inverse_root = 1.0 / math.sqrt(entries)
    dot = functools.partial(lax.dot_general, precision=lax.Precision.HIGHEST, preferred_element_type=F32)
    nn = (((1,), (0,)), ((), ()))
    tot = total[...]
    raw = tot[:, 0:KP] * inverse_root
    energy = (
        pltpu.roll(tot, TILE - KP, 1) + pltpu.roll(tot, TILE - KP - 8, 1) + pltpu.roll(tot, TILE - KP - 16, 1)
    )[:, 0:BS]
    coef = dot(raw, pq[0], nn)
    gram = (energy - dot(dot(raw, pq[1], nn), raw, NT)) * (1.0 / entries)
    coefficients[...] = coef[:, 0:KD]

    sub = lax.broadcasted_iota(jnp.int32, (BS, TILE), 0)
    lane = lax.broadcasted_iota(jnp.int32, (BS, TILE), 1)
    unit = (lane == sub + KP) | (lane == sub + KP + 8) | (lane == sub + KP + 16)
    target = jnp.where(unit, 1.0, 0.0).astype(F32)
    target = target + jnp.concatenate([coef * -inverse_root, jnp.zeros((BS, TILE - KP), F32)], axis=1)
    left = jnp.concatenate([gram, jnp.zeros((BS, TILE - BS), F32)], axis=1)
    lower = jnp.zeros((BS, TILE), F32)
    for j in range(BS):
        root = jnp.sqrt(left[j : j + 1, j : j + 1])
        scale = jnp.broadcast_to(1.0 / root, (BS, 1))
        column = jnp.broadcast_to(left[:, j : j + 1] * scale, (BS, TILE))
        below = jnp.where(sub > j, column, 0.0)
        lower = jnp.where((lane == j) & (sub >= j), column, lower)
        solved = jnp.broadcast_to(target[j : j + 1, :], (BS, TILE)) * scale
        target = jnp.where(sub == j, solved, target - below * solved)
        left = left - below * (jnp.broadcast_to(left[j : j + 1, :], (BS, TILE)) * scale)
    factor[...] = lower[:, 0:BS]
    mix = jnp.concatenate(split3(target[:, 0:STACK]), axis=0).astype(BF16)
    length = st.shape[1]
    for n in range(length // 512):
        part = slice(n * 512, (n + 1) * 512)
        wide = jnp.dot(mix, st[:, part], preferred_element_type=F32)
        new_block[:, part] = (wide[16:24] + wide[8:16]) + wide[0:8]


def shards(basis, expand, tiles, tile_rows, tile_cols):
    length = basis.shape[1]
    vmem = pl.BlockSpec(memory_space=pltpu.VMEM)
    hbm = pl.BlockSpec(memory_space=pltpu.HBM)
    dma = pltpu.SemaphoreType.DMA
    st, total, pq = pl.pallas_call(
        step_kernel,
        out_shape=(
            jax.ShapeDtypeStruct((STACK, length), BF16),
            jax.ShapeDtypeStruct((BS, TILE), F32),
            jax.ShapeDtypeStruct((2, KP, KP), F32),
        ),
        in_specs=[hbm] * 5,
        out_specs=(vmem, vmem, vmem),
        scratch_shapes=[
            pltpu.VMEM(basis.shape, BF16),
            pltpu.VMEM(expand.shape, F32),
            pltpu.SMEM(tile_rows.shape, jnp.int32),
            pltpu.SMEM(tile_cols.shape, jnp.int32),
            pltpu.VMEM(tiles.shape, BF16),
            pltpu.VMEM((ROWS, MATS, 256, TILE), BF16),
            pltpu.VMEM((ROWS * REGION, BS, TILE), F32),
            pltpu.VMEM((COLS, PER * BS, TILE), F32),
            pltpu.VMEM((COLS, PER * BS, TILE), BF16),
            pltpu.VMEM((COLS, PER * BS, TILE), BF16),
            pltpu.VMEM((COLS, SLOTS * BS, TILE), F32),
            pltpu.VMEM((REGION * BS, TILE), F32),
            pltpu.VMEM((REGION, COLS * SLOTS), BF16),
            pltpu.VMEM((COLS, SLOTS, TILE), jnp.int32),
            pltpu.VMEM((COLS, SLOTS, TILE), jnp.int32),
            pltpu.VMEM((COLS, 16, TILE), F32),
            pltpu.VMEM((ROWS, 16, TILE), F32),
            pltpu.VMEM((COLS, BS, TILE), F32),
            pltpu.VMEM((ROWS, BS, TILE), F32),
            pltpu.VMEM((KP, TILE), F32),
            dma((4,)),
            dma((MATS, 4)),
            dma((MATS, 9)), dma((MATS, 9)),
            dma((COLS,)), dma((COLS,)),
            dma((COLS,)), dma((COLS,)),
            dma((ROWS,)), dma((ROWS,)),
            dma((COLS,)), dma((COLS,)),
            dma((COLS,)), dma((COLS,)),
            dma((ROWS,)), dma((ROWS,)),
        ],
        compiler_params=pltpu.CompilerParams(
            collective_id=0, has_side_effects=True, vmem_limit_bytes=36 * 2**20
        ),
        name="toar_step",
    )(*(pltpu.with_memory_space_constraint(a, pltpu.HBM) for a in (basis, expand, tile_rows, tile_cols, tiles)))
    return tuple(
        pl.pallas_call(
            functools.partial(final_kernel, entries=length * ROWS * COLS),
            out_shape=(
                jax.ShapeDtypeStruct((BS, length), F32),
                jax.ShapeDtypeStruct((BS, KD), F32),
                jax.ShapeDtypeStruct((BS, BS), F32),
            ),
            in_specs=[vmem, vmem, vmem],
            out_specs=(vmem, vmem, vmem),
            compiler_params=pltpu.CompilerParams(vmem_limit_bytes=8 * 2**20),
            name="toar_final",
        )(st, total, pq)
    )


def solution(mesh):
    finer = Mesh(mesh.devices.reshape(SIZES), AXES)
    return jax.shard_map(
        shards,
        mesh=finer,
        in_specs=(P(None, AXES), P(), P(None, AXES, None, None), P(AXES), P(AXES)),
        out_specs=(P(None, AXES), P(), P()),
        check_vma=False,
    )
```

```python
import functools
import math

import jax
import jax.numpy as jnp
from jax import lax
from jax.experimental import pallas as pl
from jax.experimental.pallas import tpu as pltpu
from jax.sharding import Mesh
from jax.sharding import PartitionSpec as P

AXES = ("xh", "y", "xl", "z", "core")
SIZES = (2, 4, 2, 4, 2)
MESH = pl.DeviceIdType.MESH
F32, BF16 = jnp.float32, jnp.bfloat16
NT = (((1,), (1,)), ((), ()))

COLS, ROWS = 16, 8
MATS, BS, KD, TILE = 3, 8, 40, 128
REGION = 32
PER = 12
SLOTS = 16
KP = 48
COL_ORDER = (12, 13, 4, 5, 10, 11, 14, 15, 2, 3, 6, 7, 8, 9, 1)
ROW_ORDER = (6, 5, 7, 4, 2, 1, 3)
STACK = 80


def split3(value):
    high = value.astype(BF16).astype(F32)
    rest = value - high
    middle = rest.astype(BF16).astype(F32)
    return high, middle, rest - middle


def step_kernel(
    basis_hbm, expand_hbm, rows_hbm, cols_hbm, tiles, st, total, pq,
    basis, expand, rows, cols, a_vm, xb, xf, acc, ysend, yrecv, rf, app, onehot, ids_s, ids_r, c1, c2, m1, m2, cw,
    in_sem, tile_sem, g_send, g_recv, i_send, i_recv, c1_send, c1_recv, c2_send, c2_recv,
    y_send, y_recv, m1_send, m1_recv, m2_send, m2_recv,
):
    xh, y, xl, z, core = (lax.axis_index(a) for a in AXES)
    row, col = xh * 4 + y, xl * 8 + z * 2 + core

    def col_peer(j):
        px, pz, pk = lax.rem(xl + j // 8, 2), lax.rem(z + (j // 2) % 4, 4), lax.rem(core + j % 2, 2)
        return (xh, y, px, pz, pk), px * 8 + pz * 2 + pk

    def col_source(j):
        px, pz, pk = lax.rem(xl + j // 8, 2), lax.rem(z + 4 - (j // 2) % 4, 4), lax.rem(core + j % 2, 2)
        return px * 8 + pz * 2 + pk

    def row_peer(j):
        ph, py = lax.rem(xh + j // 4, 2), lax.rem(y + j % 4, 4)
        return (ph, py, xl, z, core)

    def remote(src, dst, send, recv, device):
        return pltpu.make_async_remote_copy(
            src_ref=src, dst_ref=dst, send_sem=send, recv_sem=recv, device_id=device, device_id_type=MESH
        )

    in_copies = [
        pltpu.make_async_copy(src, dst, in_sem.at[i])
        for i, (src, dst) in enumerate(
            ((basis_hbm, basis), (expand_hbm, expand), (rows_hbm, rows), (cols_hbm, cols))
        )
    ]
    for copy in in_copies:
        copy.start()
    barrier = pltpu.get_barrier_semaphore()
    for j in range(1, ROWS):
        pl.semaphore_signal(barrier, inc=1, device_id=row_peer(j), device_id_type=MESH)
    for j in range(1, COLS):
        pl.semaphore_signal(barrier, inc=1, device_id=col_peer(j)[0], device_id_type=MESH)

    in_copies[0].wait()
    in_copies[1].wait()
    tile_copies = []
    for m in range(MATS):
        for q in range(3):
            part = pl.ds(64 * q, 64)
            copy = pltpu.make_async_copy(tiles.at[m, part], a_vm.at[m, part], tile_sem.at[m, q])
            copy.start()
            tile_copies.append(copy)

    coef = jnp.concatenate([expand[m] for m in range(MATS)], axis=0)
    lhs = jnp.concatenate(split3(coef), axis=0).astype(BF16)
    for n in range(8):
        wide = jnp.dot(lhs, basis[:, n * 512 : (n + 1) * 512], preferred_element_type=F32)
        for m in range(MATS):
            a, b, c = (wide[24 * i + 8 * m : 24 * i + 8 * m + 8] for i in range(3))
            value = (c + b) + a
            for h in range(2):
                pair = jnp.concatenate(
                    [value[:, (2 * h + i) * TILE : (2 * h + i + 1) * TILE] for i in range(2)], axis=0
                )
                xb[row, m, 64 * (n // 2) + 32 * (n % 2) + 16 * h : 64 * (n // 2) + 32 * (n % 2) + 16 * h + 16, :] = pair.astype(BF16)

    pl.semaphore_wait(barrier, ROWS + COLS - 2)

    up, down = lax.rem(y + 1, 4), lax.rem(y + 3, 4)
    far, other = lax.rem(y + 2, 4), 1 - xh
    to_up, to_down, to_other = (xh, up, xl, z, core), (xh, down, xl, z, core), (other, y, xl, z, core)
    whole, first, second = pl.ds(0, 256), pl.ds(0, 128), pl.ds(128, 128)

    def gather(m, i, slot, part, device):
        ref = xb.at[slot, m, part]
        return remote(ref, ref, g_send.at[m, i], g_recv.at[m, i], device)

    def moves(m):
        return (
            gather(m, 0, row, whole, to_up),
            gather(m, 1, row, whole, to_down),
            gather(m, 2, row, whole, to_other),
            gather(m, 3, xh * 4 + down, first, to_up),
            gather(m, 4, xh * 4 + up, second, to_down),
            gather(m, 5, other * 4 + y, whole, to_up),
            gather(m, 6, other * 4 + y, whole, to_down),
            gather(m, 7, xh * 4 + far, first, to_other),
            gather(m, 8, xh * 4 + far, second, to_other),
        )

    hops = [moves(m) for m in range(MATS)]
    for m in range(MATS):
        for i in (2, 0, 1):
            hops[m][i].start()

    in_copies[2].wait()
    in_copies[3].wait()

    def fill_ids(k, carry):
        for u in range(SLOTS):
            if u < PER:
                value = rows[k * PER + u] - k * REGION
            else:
                value = jnp.int32(-1)
            ids_s[k, u : u + 1, :] = jnp.full((1, TILE), value, jnp.int32)
        return carry

    lax.fori_loop(0, COLS, fill_ids, 0)
    id_copies = []
    for j in range(1, COLS):
        device, k = col_peer(j)
        copy = remote(ids_s.at[k], ids_r.at[col], i_send.at[j], i_recv.at[j], device)
        copy.start()
        id_copies.append(copy)
    ids_r[col] = ids_s[col]

    st[0:KD, :] = basis[...]
    st[KD:KP, :] = jnp.zeros((KP - KD, st.shape[1]), BF16)
    own = lax.dot_general(st[0:KP, :], st[0:KP, :], NT, preferred_element_type=F32)
    cw[...] = jnp.zeros(cw.shape, F32)
    cw[:, 0:KP] = own
    packed = cw[0:16, :] + pltpu.roll(cw[16:32, :], 40, 1) + pltpu.roll(cw[32:48, :], 80, 1)
    c1[col] = packed
    c1_copies = []
    for j in range(1, COLS):
        device, _ = col_peer(j)
        copy = remote(c1.at[col], c1.at[col], c1_send.at[j], c1_recv.at[j], device)
        copy.start()
        c1_copies.append(copy)

    def arrive(m):
        hops[m][5].wait_recv()
        unpack(m, other * 4 + down)
        hops[m][6].wait_recv()
        unpack(m, other * 4 + up)
        hops[m][7].wait_recv()
        hops[m][8].wait_recv()
        unpack(m, other * 4 + far)

    zero = jnp.zeros((BS, TILE), F32)

    def products(m, t):
        rows_of = []
        for i in (t, t + 2):
            x0, x1 = xf[m, cols[i]], xf[m, cols[i + 1]]
            rows_of += [jnp.concatenate([x0, zero], axis=1), jnp.concatenate([zero, x1], axis=1)]
        lhs = jnp.concatenate(rows_of, axis=0).astype(BF16)
        rhs = jnp.concatenate(
            [jnp.concatenate([a_vm[m, i], a_vm[m, i + 1]], axis=0) for i in (t, t + 2)], axis=1
        )
        out = jnp.dot(lhs, rhs, preferred_element_type=F32)
        return jnp.concatenate([out[0:16, 0:TILE], out[16:32, TILE:]], axis=0)

    def pair_product(m, t):
        x0, x1 = xf[m, cols[t]], xf[m, cols[t + 1]]
        lhs = jnp.concatenate(
            [jnp.concatenate([x0, zero], axis=1), jnp.concatenate([zero, x1], axis=1)], axis=0
        ).astype(BF16)
        rhs = jnp.concatenate([a_vm[m, t], a_vm[m, t + 1]], axis=1)
        return lax.dot_general(lhs, rhs, NT, preferred_element_type=F32)

    def run_first(k, carry):
        for p in range(PER // 2):
            acc[k, 16 * p : 16 * p + 16, :] = pair_product(0, k * PER + 2 * p)
        return carry

    def run_second(k, carry):
        for p in range(PER // 2):
            acc[k, 16 * p : 16 * p + 16, :] += pair_product(1, k * PER + 2 * p)
        return carry

    def run_last(k):
        for p in range(PER // 4):
            part = slice(32 * p, 32 * p + 32)
            ysend[k, part, :] = (acc[k, part, :] + products(2, k * PER + 4 * p)).astype(BF16)

    def unpack(m, slot):
        xf[m, pl.ds(slot * REGION, REGION)] = xb[slot, m].astype(F32).reshape(REGION, BS, TILE)

    def flip(m, q):
        tile_copies[3 * m + q].wait()

        def some(i, carry):
            for u in range(16):
                t = 64 * q + 16 * i + u
                a_vm[m, t] = a_vm[m, t].T
            return carry

        lax.fori_loop(0, 4, some, 0)

    for m, h in enumerate(hops):
        h[0].wait_recv()
        h[3].start()
        h[1].wait_recv()
        h[4].start()
    for m, h in enumerate(hops):
        h[2].wait_recv()
        h[5].start()
        h[6].start()
        for slot in (row, xh * 4 + down, xh * 4 + up, other * 4 + y):
            unpack(m, slot)
    for m, h in enumerate(hops):
        h[3].wait_recv()
        h[7].start()
        h[4].wait_recv()
        h[8].start()
        unpack(m, xh * 4 + far)
        flip(2, m)

    for copy in id_copies:
        copy.wait_recv()
    lane = lax.broadcasted_iota(jnp.int32, (COLS * SLOTS, TILE), 1)
    chosen = jnp.where(ids_r[...].reshape(COLS * SLOTS, TILE) == lane, 1.0, 0.0).astype(F32)
    onehot[...] = chosen.T[0:REGION, :].astype(BF16)
    for k in range(COLS):
        rf[k, PER * BS :, :] = jnp.zeros(((SLOTS - PER) * BS, TILE), F32)

    arrive(0)
    for copy in tile_copies[0:3]:
        copy.wait()
    lax.fori_loop(0, COLS, run_first, 0, unroll=COLS)
    arrive(1)
    for copy in tile_copies[3:6]:
        copy.wait()
    lax.fori_loop(0, COLS, run_second, 0, unroll=COLS)

    arrive(2)

    def result_copy(j):
        device, k = col_peer(j)
        return remote(ysend.at[k], yrecv.at[col], y_send.at[j], y_recv.at[j], device)

    def far_first(i):
        return (1 - (i // 2) % 2) * 8 + (1 + i // 4) % 4 * 2 + 1 - i % 2

    def last(i, carry):
        j = far_first(i)
        run_last(col_peer(j)[1])
        result_copy(j).start()
        return carry

    lax.fori_loop(0, COLS - 1, last, 0, unroll=COLS - 1)
    run_last(col)

    for copy in c1_copies:
        copy.wait_recv()
    half = c1[0]
    for k in range(1, COLS):
        half = half + c1[k]
    c2[row] = half
    c2_copies = []
    for j in range(1, ROWS):
        copy = remote(c2.at[row], c2.at[row], c2_send.at[j], c2_recv.at[j], row_peer(j))
        copy.start()
        c2_copies.append(copy)

    rf[col, 0 : PER * BS, :] = ysend[col].astype(F32)

    def landed(i, carry):
        j = far_first(i)
        k = col_source(j)
        result_copy(j).wait_recv()
        rf[k, 0 : PER * BS, :] = yrecv[k].astype(F32)
        return carry

    lax.fori_loop(0, COLS - 1, landed, 0, unroll=COLS - 1)

    for b in range(0, BS, 2):
        pair = [
            jnp.concatenate([rf[k, pl.ds(b + i, SLOTS, stride=BS), :] for k in range(COLS)], axis=0) for i in range(2)
        ]
        both = jnp.dot(onehot[...], jnp.concatenate(pair, axis=1).astype(BF16), preferred_element_type=F32)
        for i in range(2):
            app[pl.ds(b + i, REGION, stride=BS), :] = both[:, i * TILE : (i + 1) * TILE]
    for s in range(REGION):
        parts = split3(app[s * BS : (s + 1) * BS, :])
        st[KP:STACK, s * TILE : (s + 1) * TILE] = jnp.concatenate([*parts, zero], axis=0).astype(BF16)

    inner = lax.dot_general(st[KP:STACK, :], st[...], NT, preferred_element_type=F32)
    m1[col, :, 0:STACK] = (inner[16:24] + inner[8:16]) + inner[0:8]
    m1[col, :, STACK:] = jnp.zeros((BS, TILE - STACK), F32)
    m1_copies = []
    for j in COL_ORDER:
        device, _ = col_peer(j)
        copy = remote(m1.at[col], m1.at[col], m1_send.at[j], m1_recv.at[j], device)
        copy.start()
        m1_copies.append(copy)
    for copy in c2_copies:
        copy.wait_recv()
    full = c2[0]
    for r in range(1, ROWS):
        full = full + c2[r]
    lanes = lax.broadcasted_iota(jnp.int32, (16, TILE), 1)
    keep = lanes < KD
    for i in range(3):
        cw[16 * i : 16 * i + 16, :] = jnp.where(keep, full if i == 0 else pltpu.roll(full, TILE - 40 * i, 1), 0.0)
    entries = float(st.shape[1] * ROWS * COLS)
    corr = cw[...] * (1.0 / entries)
    eye = jnp.where(
        lax.broadcasted_iota(jnp.int32, (KP, TILE), 0) == lax.broadcasted_iota(jnp.int32, (KP, TILE), 1), 1.0, 0.0
    ).astype(F32)
    dot = functools.partial(jnp.dot, precision=lax.Precision.HIGHEST, preferred_element_type=F32)
    corr2 = dot(corr[:, 0:KP], corr)
    corr3 = dot(corr2[:, 0:KP], corr)
    pq[...] = (2.0 * eye - corr) + pltpu.roll(4.0 * eye - 6.0 * corr + 4.0 * corr2 - corr3, TILE // 2, 1)

    for copy in m1_copies:
        copy.wait_recv()
    half = m1[0]
    for k in range(1, COLS):
        half = half + m1[k]
    m2[row] = half
    m2_copies = []
    for j in ROW_ORDER:
        copy = remote(m2.at[row], m2.at[row], m2_send.at[j], m2_recv.at[j], row_peer(j))
        copy.start()
        m2_copies.append(copy)
    for copy in m2_copies:
        copy.wait_recv()
    full = m2[0]
    for r in range(1, ROWS):
        full = full + m2[r]
    total[...] = full

    for m in range(MATS):
        for copy in hops[m]:
            copy.wait_send()
    for copy in (*id_copies, *c1_copies, *c2_copies, *m1_copies, *m2_copies):
        copy.wait_send()

    def sent(j, carry):
        result_copy(j).wait_send()
        return carry

    lax.fori_loop(1, COLS, sent, 0)


def final_kernel(st, total, pq, new_block, coefficients, factor, *, entries):
    inverse_root = 1.0 / math.sqrt(entries)
    tot = total[...]
    raw = tot * inverse_root
    both = jnp.dot(raw[:, 0:KP], pq[...], precision=lax.Precision.HIGHEST, preferred_element_type=F32)
    coefficients[...] = both[:, 0:KD]

    sub = lax.broadcasted_iota(jnp.int32, (BS, TILE), 0)
    lane = lax.broadcasted_iota(jnp.int32, (BS, TILE), 1)
    basis_part = lane < KP
    turned = jnp.where(basis_part, pltpu.roll(both, TILE // 2, 1), 0.0)

    def parts_of(index):
        return (lane == index + KP) | (lane == index + KP + 8) | (lane == index + KP + 16)

    def spread(value, j):
        return jnp.broadcast_to(value[j : j + 1, :], (BS, TILE))

    columns = [
        jnp.broadcast_to(
            jnp.sum(jnp.where(parts_of(j), tot, 0.0) - turned * spread(raw, j), axis=1, keepdims=True)
            * (1.0 / entries),
            (BS, TILE),
        )
        for j in range(BS)
    ]
    target = jnp.where(basis_part, both * -inverse_root, 0.0) + jnp.where(parts_of(sub), 1.0, 0.0)
    lower = jnp.zeros((BS, TILE), F32)
    for j in range(BS):
        pivot = spread(columns[j], j)
        scale = lax.rsqrt(pivot)
        scale = scale * (1.5 - 0.5 * pivot * scale * scale)
        column = columns[j] * scale
        below = jnp.where(sub > j, column, 0.0)
        lower = jnp.where((lane == j) & (sub >= j), column, lower)
        solved = spread(target, j) * scale
        target = jnp.where(sub == j, solved, target - below * solved)
        for i in range(j + 1, BS):
            columns[i] = columns[i] - below * spread(below, i)
    factor[...] = lower[:, 0:BS]
    mix = jnp.concatenate(split3(target[:, 0:STACK]), axis=0).astype(BF16)
    length = st.shape[1]
    for n in range(length // 512):
        part = slice(n * 512, (n + 1) * 512)
        wide = jnp.dot(mix, st[:, part], preferred_element_type=F32)
        new_block[:, part] = (wide[16:24] + wide[8:16]) + wide[0:8]


def shards(basis, expand, tiles, tile_rows, tile_cols):
    length = basis.shape[1]
    vmem = pl.BlockSpec(memory_space=pltpu.VMEM)
    hbm = pl.BlockSpec(memory_space=pltpu.HBM)
    dma = pltpu.SemaphoreType.DMA
    st, total, pq = pl.pallas_call(
        step_kernel,
        out_shape=(
            jax.ShapeDtypeStruct((STACK, length), BF16),
            jax.ShapeDtypeStruct((BS, TILE), F32),
            jax.ShapeDtypeStruct((KP, TILE), F32),
        ),
        in_specs=[hbm] * 5,
        out_specs=(vmem, vmem, vmem),
        scratch_shapes=[
            pltpu.VMEM(basis.shape, BF16),
            pltpu.VMEM(expand.shape, F32),
            pltpu.SMEM(tile_rows.shape, jnp.int32),
            pltpu.SMEM(tile_cols.shape, jnp.int32),
            pltpu.VMEM(tiles.shape, BF16),
            pltpu.VMEM((ROWS, MATS, 256, TILE), BF16),
            pltpu.VMEM((MATS, ROWS * REGION, BS, TILE), F32),
            pltpu.VMEM((COLS, PER * BS, TILE), F32),
            pltpu.VMEM((COLS, PER * BS, TILE), BF16),
            pltpu.VMEM((COLS, PER * BS, TILE), BF16),
            pltpu.VMEM((COLS, SLOTS * BS, TILE), F32),
            pltpu.VMEM((REGION * BS, TILE), F32),
            pltpu.VMEM((REGION, COLS * SLOTS), BF16),
            pltpu.VMEM((COLS, SLOTS, TILE), jnp.int32),
            pltpu.VMEM((COLS, SLOTS, TILE), jnp.int32),
            pltpu.VMEM((COLS, 16, TILE), F32),
            pltpu.VMEM((ROWS, 16, TILE), F32),
            pltpu.VMEM((COLS, BS, TILE), F32),
            pltpu.VMEM((ROWS, BS, TILE), F32),
            pltpu.VMEM((KP, TILE), F32),
            dma((4,)),
            dma((MATS, 3)),
            dma((MATS, 9)), dma((MATS, 9)),
            dma((COLS,)), dma((COLS,)),
            dma((COLS,)), dma((COLS,)),
            dma((ROWS,)), dma((ROWS,)),
            dma((COLS,)), dma((COLS,)),
            dma((COLS,)), dma((COLS,)),
            dma((ROWS,)), dma((ROWS,)),
        ],
        compiler_params=pltpu.CompilerParams(
            collective_id=0, has_side_effects=True, vmem_limit_bytes=36 * 2**20
        ),
        name="toar_step",
    )(*(pltpu.with_memory_space_constraint(a, pltpu.HBM) for a in (basis, expand, tile_rows, tile_cols, tiles)))
    return tuple(
        pl.pallas_call(
            functools.partial(final_kernel, entries=length * ROWS * COLS),
            out_shape=(
                jax.ShapeDtypeStruct((BS, length), F32),
                jax.ShapeDtypeStruct((BS, KD), F32),
                jax.ShapeDtypeStruct((BS, BS), F32),
            ),
            in_specs=[vmem, vmem, vmem],
            out_specs=(vmem, vmem, vmem),
            compiler_params=pltpu.CompilerParams(vmem_limit_bytes=8 * 2**20),
            name="toar_final",
        )(st, total, pq)
    )


def solution(mesh):
    finer = Mesh(mesh.devices.reshape(SIZES), AXES)
    return jax.shard_map(
        shards,
        mesh=finer,
        in_specs=(P(None, AXES), P(), P(None, AXES, None, None), P(AXES), P(AXES)),
        out_specs=(P(None, AXES), P(), P()),
        check_vma=False,
    )
```

```python
import functools
import math

import jax
import jax.numpy as jnp
from jax import lax
from jax.experimental import pallas as pl
from jax.experimental.pallas import tpu as pltpu
from jax.sharding import Mesh
from jax.sharding import PartitionSpec as P

AXES = ("xh", "y", "xl", "z", "core")
SIZES = (2, 4, 2, 4, 2)
MESH = pl.DeviceIdType.MESH
F32, BF16 = jnp.float32, jnp.bfloat16
NT = (((1,), (1,)), ((), ()))

COLS, ROWS = 16, 8
MATS, BS, KD, TILE = 3, 8, 40, 128
REGION = 32
PER = 12
SLOTS = 16
KP = 48
COL_ORDER = (12, 13, 4, 5, 10, 11, 14, 15, 2, 3, 6, 7, 8, 9, 1)
ROW_ORDER = (6, 5, 7, 4, 2, 1, 3)
STACK = 80


def split3(value):
    high = value.astype(BF16).astype(F32)
    rest = value - high
    middle = rest.astype(BF16).astype(F32)
    return high, middle, rest - middle


def step_kernel(
    basis_hbm, expand_hbm, rows_hbm, cols_hbm, tiles, st, total, pq,
    basis, expand, rows, cols, a_vm, xb, xf, acc, ysend, yrecv, rf, app, onehot, ids_s, ids_r, c1, c2, m1, m2, cw,
    in_sem, tile_sem, g_send, g_recv, i_send, i_recv, c1_send, c1_recv, c2_send, c2_recv,
    y_send, y_recv, m1_send, m1_recv, m2_send, m2_recv,
):
    xh, y, xl, z, core = (lax.axis_index(a) for a in AXES)
    row, col = xh * 4 + y, xl * 8 + z * 2 + core

    def col_peer(j):
        px, pz, pk = lax.rem(xl + j // 8, 2), lax.rem(z + (j // 2) % 4, 4), lax.rem(core + j % 2, 2)
        return (xh, y, px, pz, pk), px * 8 + pz * 2 + pk

    def far_first(i):
        return (1 - (i // 2) % 2) * 8 + (1 + i // 4) % 4 * 2 + 1 - i % 2

    def row_peer(j):
        ph, py = lax.rem(xh + j // 4, 2), lax.rem(y + j % 4, 4)
        return (ph, py, xl, z, core)

    def remote(src, dst, send, recv, device):
        return pltpu.make_async_remote_copy(
            src_ref=src, dst_ref=dst, send_sem=send, recv_sem=recv, device_id=device, device_id_type=MESH
        )

    in_copies = [
        pltpu.make_async_copy(src, dst, in_sem.at[i])
        for i, (src, dst) in enumerate(
            ((basis_hbm, basis), (expand_hbm, expand), (rows_hbm, rows), (cols_hbm, cols))
        )
    ]
    for copy in in_copies:
        copy.start()
    barrier = pltpu.get_barrier_semaphore()
    for j in range(1, ROWS):
        pl.semaphore_signal(barrier, inc=1, device_id=row_peer(j), device_id_type=MESH)
    for j in range(1, COLS):
        pl.semaphore_signal(barrier, inc=1, device_id=col_peer(j)[0], device_id_type=MESH)

    in_copies[0].wait()
    in_copies[1].wait()
    tile_copies = []
    for m in range(MATS):
        for q in range(3):
            part = pl.ds(64 * q, 64)
            copy = pltpu.make_async_copy(tiles.at[m, part], a_vm.at[m, part], tile_sem.at[m, q])
            copy.start()
            tile_copies.append(copy)

    coef = jnp.concatenate([expand[m] for m in range(MATS)], axis=0)
    lhs = jnp.concatenate(split3(coef), axis=0).astype(BF16)
    for n in range(8):
        wide = jnp.dot(lhs, basis[:, n * 512 : (n + 1) * 512], preferred_element_type=F32)
        for m in range(MATS):
            a, b, c = (wide[24 * i + 8 * m : 24 * i + 8 * m + 8] for i in range(3))
            value = (c + b) + a
            for h in range(2):
                pair = jnp.concatenate(
                    [value[:, (2 * h + i) * TILE : (2 * h + i + 1) * TILE] for i in range(2)], axis=0
                )
                xb[row, m, 64 * (n // 2) + 32 * (n % 2) + 16 * h : 64 * (n // 2) + 32 * (n % 2) + 16 * h + 16, :] = pair.astype(BF16)

    pl.semaphore_wait(barrier, ROWS + COLS - 2)

    up, down = lax.rem(y + 1, 4), lax.rem(y + 3, 4)
    far, other = lax.rem(y + 2, 4), 1 - xh
    to_up, to_down, to_other = (xh, up, xl, z, core), (xh, down, xl, z, core), (other, y, xl, z, core)
    whole, first, second = pl.ds(0, 256), pl.ds(0, 128), pl.ds(128, 128)

    def gather(m, i, slot, part, device):
        ref = xb.at[slot, m, part]
        return remote(ref, ref, g_send.at[m, i], g_recv.at[m, i], device)

    def moves(m):
        return (
            gather(m, 0, row, whole, to_up),
            gather(m, 1, row, whole, to_down),
            gather(m, 2, row, whole, to_other),
            gather(m, 3, xh * 4 + down, first, to_up),
            gather(m, 4, xh * 4 + up, second, to_down),
            gather(m, 5, other * 4 + y, whole, to_up),
            gather(m, 6, other * 4 + y, whole, to_down),
            gather(m, 7, xh * 4 + far, first, to_other),
            gather(m, 8, xh * 4 + far, second, to_other),
        )

    hops = [moves(m) for m in range(MATS)]
    for m in range(MATS):
        for i in (2, 0, 1):
            hops[m][i].start()

    in_copies[2].wait()
    in_copies[3].wait()

    def fill_ids(k, carry):
        for u in range(SLOTS):
            if u < PER:
                value = rows[k * PER + u] - k * REGION
            else:
                value = jnp.int32(-1)
            ids_s[k, u : u + 1, :] = jnp.full((1, TILE), value, jnp.int32)
        return carry

    lax.fori_loop(0, COLS, fill_ids, 0)
    id_copies = []
    for i in range(COLS - 1):
        device, k = col_peer(far_first(i))
        copy = remote(ids_s.at[k], ids_r.at[i], i_send.at[i], i_recv.at[i], device)
        copy.start()
        id_copies.append(copy)
    ids_r[COLS - 1] = ids_s[col]

    st[0:KD, :] = basis[...]
    st[KD:KP, :] = jnp.zeros((KP - KD, st.shape[1]), BF16)
    own = lax.dot_general(st[0:KP, :], st[0:KP, :], NT, preferred_element_type=F32)
    cw[...] = jnp.zeros(cw.shape, F32)
    cw[:, 0:KP] = own
    packed = cw[0:16, :] + pltpu.roll(cw[16:32, :], 40, 1) + pltpu.roll(cw[32:48, :], 80, 1)
    c1[col] = packed
    c1_copies = []
    for j in range(1, COLS):
        device, _ = col_peer(j)
        copy = remote(c1.at[col], c1.at[col], c1_send.at[j], c1_recv.at[j], device)
        copy.start()
        c1_copies.append(copy)

    def arrive(m):
        hops[m][5].wait_recv()
        unpack(m, other * 4 + down)
        hops[m][6].wait_recv()
        unpack(m, other * 4 + up)
        hops[m][7].wait_recv()
        hops[m][8].wait_recv()
        unpack(m, other * 4 + far)

    zero = jnp.zeros((BS, TILE), F32)

    def products(m, t):
        rows_of = []
        for i in (t, t + 2):
            x0, x1 = xf[m, cols[i]], xf[m, cols[i + 1]]
            rows_of += [jnp.concatenate([x0, zero], axis=1), jnp.concatenate([zero, x1], axis=1)]
        lhs = jnp.concatenate(rows_of, axis=0).astype(BF16)
        rhs = jnp.concatenate(
            [jnp.concatenate([a_vm[m, i], a_vm[m, i + 1]], axis=0) for i in (t, t + 2)], axis=1
        )
        out = jnp.dot(lhs, rhs, preferred_element_type=F32)
        return jnp.concatenate([out[0:16, 0:TILE], out[16:32, TILE:]], axis=0)

    def pair_product(m, t):
        x0, x1 = xf[m, cols[t]], xf[m, cols[t + 1]]
        lhs = jnp.concatenate(
            [jnp.concatenate([x0, zero], axis=1), jnp.concatenate([zero, x1], axis=1)], axis=0
        ).astype(BF16)
        rhs = jnp.concatenate([a_vm[m, t], a_vm[m, t + 1]], axis=1)
        return lax.dot_general(lhs, rhs, NT, preferred_element_type=F32)

    def run_first(k, carry):
        for p in range(PER // 4):
            acc[k, 32 * p : 32 * p + 32, :] = products(0, k * PER + 4 * p)
        return carry

    def run_second(k, carry):
        for p in range(PER // 2):
            acc[k, 16 * p : 16 * p + 16, :] += pair_product(1, k * PER + 2 * p)
        return carry

    def run_last(k):
        for p in range(PER // 4):
            part = slice(32 * p, 32 * p + 32)
            ysend[k, part, :] = (acc[k, part, :] + products(2, k * PER + 4 * p)).astype(BF16)

    def unpack(m, slot):
        xf[m, pl.ds(slot * REGION, REGION)] = xb[slot, m].astype(F32).reshape(REGION, BS, TILE)

    def flip(m, q):
        tile_copies[3 * m + q].wait()

        def some(i, carry):
            for u in range(32):
                t = 64 * q + 32 * i + u
                a_vm[m, t] = a_vm[m, t].T
            return carry

        lax.fori_loop(0, 2, some, 0)

    for m, h in enumerate(hops):
        h[0].wait_recv()
        h[3].start()
        h[1].wait_recv()
        h[4].start()
        flip(0, m)
    for m, h in enumerate(hops):
        h[2].wait_recv()
        h[5].start()
        h[6].start()
        for slot in (row, xh * 4 + down, xh * 4 + up, other * 4 + y):
            unpack(m, slot)
    for m, h in enumerate(hops):
        h[3].wait_recv()
        h[7].start()
        h[4].wait_recv()
        h[8].start()
        unpack(m, xh * 4 + far)
        flip(2, m)

    for copy in id_copies:
        copy.wait_recv()
    lane = lax.broadcasted_iota(jnp.int32, (COLS * SLOTS, TILE), 1)
    chosen = jnp.where(ids_r[...].reshape(COLS * SLOTS, TILE) == lane, 1.0, 0.0).astype(F32)
    onehot[...] = chosen.T[0:REGION, :].astype(BF16)
    for k in range(COLS):
        rf[k, PER * BS :, :] = jnp.zeros(((SLOTS - PER) * BS, TILE), F32)

    arrive(0)
    lax.fori_loop(0, COLS, run_first, 0, unroll=COLS)
    arrive(1)
    for copy in tile_copies[3:6]:
        copy.wait()
    lax.fori_loop(0, COLS, run_second, 0, unroll=COLS)

    arrive(2)

    def result_copy(i):
        device, k = col_peer(far_first(i))
        return remote(ysend.at[k], yrecv.at[i], y_send.at[i], y_recv.at[i], device)

    def last(i, carry):
        run_last(col_peer(far_first(i))[1])
        result_copy(i).start()
        return carry

    lax.fori_loop(0, COLS - 1, last, 0, unroll=COLS - 1)
    run_last(col)

    for copy in c1_copies:
        copy.wait_recv()
    half = c1[0]
    for k in range(1, COLS):
        half = half + c1[k]
    c2[row] = half
    c2_copies = []
    for j in range(1, ROWS):
        copy = remote(c2.at[row], c2.at[row], c2_send.at[j], c2_recv.at[j], row_peer(j))
        copy.start()
        c2_copies.append(copy)

    rf[COLS - 1, 0 : PER * BS, :] = ysend[col].astype(F32)

    def landed(i, carry):
        result_copy(i).wait_recv()
        rf[i, 0 : PER * BS, :] = yrecv[i].astype(F32)
        return carry

    half_cols = COLS // 2
    for g in range(2):
        lax.fori_loop(g * half_cols, min((g + 1) * half_cols, COLS - 1), landed, 0, unroll=half_cols - g)
        group = range(g * half_cols, (g + 1) * half_cols)
        for b in range(0, BS, 2):
            pair = [
                jnp.concatenate([rf[k, pl.ds(b + i, SLOTS, stride=BS), :] for k in group], axis=0) for i in range(2)
            ]
            both = jnp.dot(
                onehot[:, g * half_cols * SLOTS : (g + 1) * half_cols * SLOTS],
                jnp.concatenate(pair, axis=1).astype(BF16),
                preferred_element_type=F32,
            )
            for i in range(2):
                value = both[:, i * TILE : (i + 1) * TILE]
                place = pl.ds(b + i, REGION, stride=BS)
                app[place, :] = value if g == 0 else app[place, :] + value
    for s in range(REGION):
        parts = split3(app[s * BS : (s + 1) * BS, :])
        st[KP:STACK, s * TILE : (s + 1) * TILE] = jnp.concatenate([*parts, zero], axis=0).astype(BF16)

    inner = lax.dot_general(st[KP:STACK, :], st[...], NT, preferred_element_type=F32)
    m1[col, :, 0:STACK] = (inner[16:24] + inner[8:16]) + inner[0:8]
    m1[col, :, STACK:] = jnp.zeros((BS, TILE - STACK), F32)
    m1_copies = []
    for j in COL_ORDER:
        device, _ = col_peer(j)
        copy = remote(m1.at[col], m1.at[col], m1_send.at[j], m1_recv.at[j], device)
        copy.start()
        m1_copies.append(copy)
    for copy in c2_copies:
        copy.wait_recv()
    full = c2[0]
    for r in range(1, ROWS):
        full = full + c2[r]
    lanes = lax.broadcasted_iota(jnp.int32, (16, TILE), 1)
    keep = lanes < KD
    for i in range(3):
        cw[16 * i : 16 * i + 16, :] = jnp.where(keep, full if i == 0 else pltpu.roll(full, TILE - 40 * i, 1), 0.0)
    entries = float(st.shape[1] * ROWS * COLS)
    corr = cw[...] * (1.0 / entries)
    eye = jnp.where(
        lax.broadcasted_iota(jnp.int32, (KP, TILE), 0) == lax.broadcasted_iota(jnp.int32, (KP, TILE), 1), 1.0, 0.0
    ).astype(F32)
    dot = functools.partial(jnp.dot, precision=lax.Precision.HIGHEST, preferred_element_type=F32)
    corr2 = dot(corr[:, 0:KP], corr)
    corr3 = dot(corr2[:, 0:KP], corr)
    pq[...] = (2.0 * eye - corr) + pltpu.roll(4.0 * eye - 6.0 * corr + 4.0 * corr2 - corr3, TILE // 2, 1)

    for copy in m1_copies:
        copy.wait_recv()
    half = m1[0]
    for k in range(1, COLS):
        half = half + m1[k]
    m2[row] = half
    m2_copies = []
    for j in ROW_ORDER:
        copy = remote(m2.at[row], m2.at[row], m2_send.at[j], m2_recv.at[j], row_peer(j))
        copy.start()
        m2_copies.append(copy)
    for copy in m2_copies:
        copy.wait_recv()
    full = m2[0]
    for r in range(1, ROWS):
        full = full + m2[r]
    total[...] = full

    for m in range(MATS):
        for copy in hops[m]:
            copy.wait_send()
    for copy in (*id_copies, *c1_copies, *c2_copies, *m1_copies, *m2_copies):
        copy.wait_send()

    def sent(i, carry):
        result_copy(i).wait_send()
        return carry

    lax.fori_loop(0, COLS - 1, sent, 0)


def final_kernel(st, total, pq, new_block, coefficients, factor, *, entries):
    inverse_root = 1.0 / math.sqrt(entries)
    tot = total[...]
    raw = tot * inverse_root
    both = jnp.dot(raw[:, 0:KP], pq[...], precision=lax.Precision.HIGHEST, preferred_element_type=F32)
    coefficients[...] = both[:, 0:KD]

    sub = lax.broadcasted_iota(jnp.int32, (BS, TILE), 0)
    lane = lax.broadcasted_iota(jnp.int32, (BS, TILE), 1)
    basis_part = lane < KP
    turned = jnp.where(basis_part, pltpu.roll(both, TILE // 2, 1), 0.0)

    def parts_of(index):
        return (lane == index + KP) | (lane == index + KP + 8) | (lane == index + KP + 16)

    def spread(value, j):
        return jnp.broadcast_to(value[j : j + 1, :], (BS, TILE))

    columns = [
        jnp.broadcast_to(
            jnp.sum(jnp.where(parts_of(j), tot, 0.0) - turned * spread(raw, j), axis=1, keepdims=True)
            * (1.0 / entries),
            (BS, TILE),
        )
        for j in range(BS)
    ]
    target = jnp.where(basis_part, both * -inverse_root, 0.0) + jnp.where(parts_of(sub), 1.0, 0.0)
    lower = jnp.zeros((BS, TILE), F32)
    for j in range(BS):
        pivot = spread(columns[j], j)
        scale = lax.rsqrt(pivot)
        scale = scale * (1.5 - 0.5 * pivot * scale * scale)
        column = columns[j] * scale
        below = jnp.where(sub > j, column, 0.0)
        lower = jnp.where((lane == j) & (sub >= j), column, lower)
        solved = spread(target, j) * scale
        target = jnp.where(sub == j, solved, target - below * solved)
        for i in range(j + 1, BS):
            columns[i] = columns[i] - below * spread(below, i)
    factor[...] = lower[:, 0:BS]
    mix = jnp.concatenate(split3(target[:, 0:STACK]), axis=0).astype(BF16)
    length = st.shape[1]
    for n in range(length // 512):
        part = slice(n * 512, (n + 1) * 512)
        wide = jnp.dot(mix, st[:, part], preferred_element_type=F32)
        new_block[:, part] = (wide[16:24] + wide[8:16]) + wide[0:8]


def shards(basis, expand, tiles, tile_rows, tile_cols):
    length = basis.shape[1]
    vmem = pl.BlockSpec(memory_space=pltpu.VMEM)
    hbm = pl.BlockSpec(memory_space=pltpu.HBM)
    dma = pltpu.SemaphoreType.DMA
    st, total, pq = pl.pallas_call(
        step_kernel,
        out_shape=(
            jax.ShapeDtypeStruct((STACK, length), BF16),
            jax.ShapeDtypeStruct((BS, TILE), F32),
            jax.ShapeDtypeStruct((KP, TILE), F32),
        ),
        in_specs=[hbm] * 5,
        out_specs=(vmem, vmem, vmem),
        scratch_shapes=[
            pltpu.VMEM(basis.shape, BF16),
            pltpu.VMEM(expand.shape, F32),
            pltpu.SMEM(tile_rows.shape, jnp.int32),
            pltpu.SMEM(tile_cols.shape, jnp.int32),
            pltpu.VMEM(tiles.shape, BF16),
            pltpu.VMEM((ROWS, MATS, 256, TILE), BF16),
            pltpu.VMEM((MATS, ROWS * REGION, BS, TILE), F32),
            pltpu.VMEM((COLS, PER * BS, TILE), F32),
            pltpu.VMEM((COLS, PER * BS, TILE), BF16),
            pltpu.VMEM((COLS, PER * BS, TILE), BF16),
            pltpu.VMEM((COLS, SLOTS * BS, TILE), F32),
            pltpu.VMEM((REGION * BS, TILE), F32),
            pltpu.VMEM((REGION, COLS * SLOTS), BF16),
            pltpu.VMEM((COLS, SLOTS, TILE), jnp.int32),
            pltpu.VMEM((COLS, SLOTS, TILE), jnp.int32),
            pltpu.VMEM((COLS, 16, TILE), F32),
            pltpu.VMEM((ROWS, 16, TILE), F32),
            pltpu.VMEM((COLS, BS, TILE), F32),
            pltpu.VMEM((ROWS, BS, TILE), F32),
            pltpu.VMEM((KP, TILE), F32),
            dma((4,)),
            dma((MATS, 3)),
            dma((MATS, 9)), dma((MATS, 9)),
            dma((COLS,)), dma((COLS,)),
            dma((COLS,)), dma((COLS,)),
            dma((ROWS,)), dma((ROWS,)),
            dma((COLS,)), dma((COLS,)),
            dma((COLS,)), dma((COLS,)),
            dma((ROWS,)), dma((ROWS,)),
        ],
        compiler_params=pltpu.CompilerParams(
            collective_id=0, has_side_effects=True, vmem_limit_bytes=36 * 2**20
        ),
        name="toar_step",
    )(*(pltpu.with_memory_space_constraint(a, pltpu.HBM) for a in (basis, expand, tile_rows, tile_cols, tiles)))
    return tuple(
        pl.pallas_call(
            functools.partial(final_kernel, entries=length * ROWS * COLS),
            out_shape=(
                jax.ShapeDtypeStruct((BS, length), F32),
                jax.ShapeDtypeStruct((BS, KD), F32),
                jax.ShapeDtypeStruct((BS, BS), F32),
            ),
            in_specs=[vmem, vmem, vmem],
            out_specs=(vmem, vmem, vmem),
            compiler_params=pltpu.CompilerParams(vmem_limit_bytes=8 * 2**20),
            name="toar_final",
        )(st, total, pq)
    )


def solution(mesh):
    finer = Mesh(mesh.devices.reshape(SIZES), AXES)
    return jax.shard_map(
        shards,
        mesh=finer,
        in_specs=(P(None, AXES), P(), P(None, AXES, None, None), P(AXES), P(AXES)),
        out_specs=(P(None, AXES), P(), P()),
        check_vma=False,
    )
```

```python
import functools
import math

import jax
import jax.numpy as jnp
from jax import lax
from jax.experimental import pallas as pl
from jax.experimental.pallas import tpu as pltpu
from jax.sharding import Mesh
from jax.sharding import PartitionSpec as P

AXES = ("xh", "y", "xl", "z", "core")
SIZES = (2, 4, 2, 4, 2)
MESH = pl.DeviceIdType.MESH
F32, BF16 = jnp.float32, jnp.bfloat16
NT = (((1,), (1,)), ((), ()))

COLS, ROWS = 16, 8
MATS, BS, KD, TILE = 3, 8, 40, 128
REGION = 32
PER = 12
SLOTS = 16
KP = 48
COL_ORDER = (12, 13, 4, 5, 10, 11, 14, 15, 2, 3, 6, 7, 8, 9, 1)
ROW_ORDER = (6, 5, 7, 4, 2, 1, 3)
STACK = 80


def split3(value):
    high = value.astype(BF16).astype(F32)
    rest = value - high
    middle = rest.astype(BF16).astype(F32)
    return high, middle, rest - middle


def step_kernel(
    basis_hbm, expand_hbm, rows_hbm, cols_hbm, tiles, st, total, pq,
    basis, expand, rows, cols, a_vm, xb, xf, acc, ysend, yrecv, rf, app, onehot, ids_s, ids_r, c1, c2, m1, m2, cw,
    in_sem, tile_sem, g_send, g_recv, i_send, i_recv, c1_send, c1_recv, c2_send, c2_recv,
    y_send, y_recv, m1_send, m1_recv, m2_send, m2_recv,
):
    xh, y, xl, z, core = (lax.axis_index(a) for a in AXES)
    row, col = xh * 4 + y, xl * 8 + z * 2 + core

    def col_peer(j):
        px, pz, pk = lax.rem(xl + j // 8, 2), lax.rem(z + (j // 2) % 4, 4), lax.rem(core + j % 2, 2)
        return (xh, y, px, pz, pk), px * 8 + pz * 2 + pk

    def far_first(i):
        return (1 - (i // 2) % 2) * 8 + (1 + i // 4) % 4 * 2 + 1 - i % 2

    def row_peer(j):
        ph, py = lax.rem(xh + j // 4, 2), lax.rem(y + j % 4, 4)
        return (ph, py, xl, z, core)

    def remote(src, dst, send, recv, device):
        return pltpu.make_async_remote_copy(
            src_ref=src, dst_ref=dst, send_sem=send, recv_sem=recv, device_id=device, device_id_type=MESH
        )

    in_copies = [
        pltpu.make_async_copy(src, dst, in_sem.at[i])
        for i, (src, dst) in enumerate(
            ((basis_hbm, basis), (expand_hbm, expand), (rows_hbm, rows), (cols_hbm, cols))
        )
    ]
    for copy in in_copies:
        copy.start()
    barrier = pltpu.get_barrier_semaphore()
    for j in ROW_ORDER:
        pl.semaphore_signal(barrier, inc=1, device_id=row_peer(j), device_id_type=MESH)
    for i in range(COLS - 1):
        pl.semaphore_signal(barrier, inc=1, device_id=col_peer(far_first(i))[0], device_id_type=MESH)

    in_copies[0].wait()
    in_copies[1].wait()
    tile_copies = []
    for m in range(MATS):
        for q in range(3):
            part = pl.ds(64 * q, 64)
            copy = pltpu.make_async_copy(tiles.at[m, part], a_vm.at[m, part], tile_sem.at[m, q])
            copy.start()
            tile_copies.append(copy)

    coef = jnp.concatenate([expand[m] for m in range(MATS)], axis=0)
    lhs = jnp.concatenate(split3(coef), axis=0).astype(BF16)
    for n in range(8):
        wide = jnp.dot(lhs, basis[:, n * 512 : (n + 1) * 512], preferred_element_type=F32)
        for m in range(MATS):
            a, b, c = (wide[24 * i + 8 * m : 24 * i + 8 * m + 8] for i in range(3))
            value = (c + b) + a
            for h in range(2):
                pair = jnp.concatenate(
                    [value[:, (2 * h + i) * TILE : (2 * h + i + 1) * TILE] for i in range(2)], axis=0
                )
                xb[row, m, 64 * (n // 2) + 32 * (n % 2) + 16 * h : 64 * (n // 2) + 32 * (n % 2) + 16 * h + 16, :] = pair.astype(BF16)

    pl.semaphore_wait(barrier, ROWS + COLS - 2)

    up, down = lax.rem(y + 1, 4), lax.rem(y + 3, 4)
    far, other = lax.rem(y + 2, 4), 1 - xh
    to_up, to_down, to_other = (xh, up, xl, z, core), (xh, down, xl, z, core), (other, y, xl, z, core)
    whole, first, second = pl.ds(0, 256), pl.ds(0, 128), pl.ds(128, 128)

    def gather(m, i, slot, part, device):
        ref = xb.at[slot, m, part]
        return remote(ref, ref, g_send.at[m, i], g_recv.at[m, i], device)

    def moves(m):
        return (
            gather(m, 0, row, whole, to_up),
            gather(m, 1, row, whole, to_down),
            gather(m, 2, row, whole, to_other),
            gather(m, 3, xh * 4 + down, first, to_up),
            gather(m, 4, xh * 4 + up, second, to_down),
            gather(m, 5, other * 4 + y, whole, to_up),
            gather(m, 6, other * 4 + y, whole, to_down),
            gather(m, 7, xh * 4 + far, first, to_other),
            gather(m, 8, xh * 4 + far, second, to_other),
        )

    hops = [moves(m) for m in range(MATS)]
    for m in range(MATS):
        for i in (2, 0, 1):
            hops[m][i].start()

    in_copies[2].wait()
    in_copies[3].wait()

    def fill_ids(k, carry):
        for u in range(SLOTS):
            if u < PER:
                value = rows[k * PER + u] - k * REGION
            else:
                value = jnp.int32(-1)
            ids_s[k, u : u + 1, :] = jnp.full((1, TILE), value, jnp.int32)
        return carry

    lax.fori_loop(0, COLS, fill_ids, 0)
    id_copies = []
    for i in range(COLS - 1):
        device, k = col_peer(far_first(i))
        copy = remote(ids_s.at[k], ids_r.at[i], i_send.at[i], i_recv.at[i], device)
        copy.start()
        id_copies.append(copy)
    ids_r[COLS - 1] = ids_s[col]

    st[0:KD, :] = basis[...]
    st[KD:KP, :] = jnp.zeros((KP - KD, st.shape[1]), BF16)
    own = lax.dot_general(st[0:KP, :], st[0:KP, :], NT, preferred_element_type=F32)
    cw[...] = jnp.zeros(cw.shape, F32)
    cw[:, 0:KP] = own
    packed = cw[0:16, :] + pltpu.roll(cw[16:32, :], 40, 1) + pltpu.roll(cw[32:48, :], 80, 1)
    c1[col] = packed
    def unpack(m, slot):
        xf[m, pl.ds(slot * REGION, REGION)] = xb[slot, m].astype(F32).reshape(REGION, BS, TILE)

    def flip(m, q):
        tile_copies[3 * m + q].wait()

        def some(i, carry):
            for u in range(32):
                t = 64 * q + 32 * i + u
                a_vm[m, t] = a_vm[m, t].T
            return carry

        lax.fori_loop(0, 2, some, 0)

    for m, h in enumerate(hops):
        h[0].wait_recv()
        h[3].start()
        h[1].wait_recv()
        h[4].start()
        flip(0, m)
    for m, h in enumerate(hops):
        h[2].wait_recv()
        h[5].start()
        h[6].start()
        for slot in (row, xh * 4 + down, xh * 4 + up, other * 4 + y):
            unpack(m, slot)
    for m, h in enumerate(hops):
        h[3].wait_recv()
        h[7].start()
        h[4].wait_recv()
        h[8].start()
        unpack(m, xh * 4 + far)
        flip(2, m)

    c1_copies = []
    for j in range(1, COLS):
        device, _ = col_peer(j)
        copy = remote(c1.at[col], c1.at[col], c1_send.at[j], c1_recv.at[j], device)
        copy.start()
        c1_copies.append(copy)

    def arrive(m):
        hops[m][5].wait_recv()
        unpack(m, other * 4 + down)
        hops[m][6].wait_recv()
        unpack(m, other * 4 + up)
        hops[m][7].wait_recv()
        hops[m][8].wait_recv()
        unpack(m, other * 4 + far)

    zero = jnp.zeros((BS, TILE), F32)

    def products(m, t):
        rows_of = []
        for i in (t, t + 2):
            x0, x1 = xf[m, cols[i]], xf[m, cols[i + 1]]
            rows_of += [jnp.concatenate([x0, zero], axis=1), jnp.concatenate([zero, x1], axis=1)]
        lhs = jnp.concatenate(rows_of, axis=0).astype(BF16)
        rhs = jnp.concatenate(
            [jnp.concatenate([a_vm[m, i], a_vm[m, i + 1]], axis=0) for i in (t, t + 2)], axis=1
        )
        out = jnp.dot(lhs, rhs, preferred_element_type=F32)
        return jnp.concatenate([out[0:16, 0:TILE], out[16:32, TILE:]], axis=0)

    def pair_product(m, t):
        x0, x1 = xf[m, cols[t]], xf[m, cols[t + 1]]
        lhs = jnp.concatenate(
            [jnp.concatenate([x0, zero], axis=1), jnp.concatenate([zero, x1], axis=1)], axis=0
        ).astype(BF16)
        rhs = jnp.concatenate([a_vm[m, t], a_vm[m, t + 1]], axis=1)
        return lax.dot_general(lhs, rhs, NT, preferred_element_type=F32)

    def run_first(k, carry):
        for p in range(PER // 4):
            acc[k, 32 * p : 32 * p + 32, :] = products(0, k * PER + 4 * p)
        return carry

    def run_second(k, carry):
        for p in range(PER // 2):
            acc[k, 16 * p : 16 * p + 16, :] += pair_product(1, k * PER + 2 * p)
        return carry

    def run_last(k):
        for p in range(PER // 4):
            part = slice(32 * p, 32 * p + 32)
            ysend[k, part, :] = (acc[k, part, :] + products(2, k * PER + 4 * p)).astype(BF16)

    for copy in id_copies:
        copy.wait_recv()
    lane = lax.broadcasted_iota(jnp.int32, (COLS * SLOTS, TILE), 1)
    chosen = jnp.where(ids_r[...].reshape(COLS * SLOTS, TILE) == lane, 1.0, 0.0).astype(F32)
    onehot[...] = chosen.T[0:REGION, :].astype(BF16)
    for k in range(COLS):
        rf[k, PER * BS :, :] = jnp.zeros(((SLOTS - PER) * BS, TILE), F32)

    arrive(0)
    lax.fori_loop(0, COLS, run_first, 0, unroll=COLS)
    arrive(1)
    for copy in tile_copies[3:6]:
        copy.wait()
    lax.fori_loop(0, COLS, run_second, 0, unroll=COLS)

    arrive(2)

    def result_copy(i):
        device, k = col_peer(far_first(i))
        return remote(ysend.at[k], yrecv.at[i], y_send.at[i], y_recv.at[i], device)

    def last(i, carry):
        run_last(col_peer(far_first(i))[1])
        result_copy(i).start()
        return carry

    lax.fori_loop(0, COLS - 1, last, 0, unroll=COLS - 1)
    run_last(col)

    for copy in c1_copies:
        copy.wait_recv()
    half = c1[0]
    for k in range(1, COLS):
        half = half + c1[k]
    c2[row] = half
    c2_copies = []
    for j in range(1, ROWS):
        copy = remote(c2.at[row], c2.at[row], c2_send.at[j], c2_recv.at[j], row_peer(j))
        copy.start()
        c2_copies.append(copy)

    rf[COLS - 1, 0 : PER * BS, :] = ysend[col].astype(F32)

    def landed(i, carry):
        result_copy(i).wait_recv()
        rf[i, 0 : PER * BS, :] = yrecv[i].astype(F32)
        return carry

    half_cols = COLS // 2
    for g in range(2):
        lax.fori_loop(g * half_cols, min((g + 1) * half_cols, COLS - 1), landed, 0, unroll=half_cols - g)
        group = range(g * half_cols, (g + 1) * half_cols)
        for b in range(0, BS, 2):
            pair = [
                jnp.concatenate([rf[k, pl.ds(b + i, SLOTS, stride=BS), :] for k in group], axis=0) for i in range(2)
            ]
            both = jnp.dot(
                onehot[:, g * half_cols * SLOTS : (g + 1) * half_cols * SLOTS],
                jnp.concatenate(pair, axis=1).astype(BF16),
                preferred_element_type=F32,
            )
            for i in range(2):
                value = both[:, i * TILE : (i + 1) * TILE]
                place = pl.ds(b + i, REGION, stride=BS)
                app[place, :] = value if g == 0 else app[place, :] + value
    for s in range(REGION):
        parts = split3(app[s * BS : (s + 1) * BS, :])
        st[KP:STACK, s * TILE : (s + 1) * TILE] = jnp.concatenate([*parts, zero], axis=0).astype(BF16)

    inner = lax.dot_general(st[KP:STACK, :], st[...], NT, preferred_element_type=F32)
    m1[col, :, 0:STACK] = (inner[16:24] + inner[8:16]) + inner[0:8]
    m1[col, :, STACK:] = jnp.zeros((BS, TILE - STACK), F32)
    m1_copies = []
    for j in COL_ORDER:
        device, _ = col_peer(j)
        copy = remote(m1.at[col], m1.at[col], m1_send.at[j], m1_recv.at[j], device)
        copy.start()
        m1_copies.append(copy)
    for copy in c2_copies:
        copy.wait_recv()
    full = c2[0]
    for r in range(1, ROWS):
        full = full + c2[r]
    lanes = lax.broadcasted_iota(jnp.int32, (16, TILE), 1)
    keep = lanes < KD
    for i in range(3):
        cw[16 * i : 16 * i + 16, :] = jnp.where(keep, full if i == 0 else pltpu.roll(full, TILE - 40 * i, 1), 0.0)
    entries = float(st.shape[1] * ROWS * COLS)
    corr = cw[...] * (1.0 / entries)
    eye = jnp.where(
        lax.broadcasted_iota(jnp.int32, (KP, TILE), 0) == lax.broadcasted_iota(jnp.int32, (KP, TILE), 1), 1.0, 0.0
    ).astype(F32)
    dot = functools.partial(jnp.dot, precision=lax.Precision.HIGHEST, preferred_element_type=F32)
    corr2 = dot(corr[:, 0:KP], corr)
    corr3 = dot(corr2[:, 0:KP], corr)
    pq[...] = (2.0 * eye - corr) + pltpu.roll(4.0 * eye - 6.0 * corr + 4.0 * corr2 - corr3, TILE // 2, 1)

    for copy in m1_copies:
        copy.wait_recv()
    half = m1[0]
    for k in range(1, COLS):
        half = half + m1[k]
    m2[row] = half
    m2_copies = []
    for j in ROW_ORDER:
        copy = remote(m2.at[row], m2.at[row], m2_send.at[j], m2_recv.at[j], row_peer(j))
        copy.start()
        m2_copies.append(copy)
    for copy in m2_copies:
        copy.wait_recv()
    full = m2[0]
    for r in range(1, ROWS):
        full = full + m2[r]
    total[...] = full

    for m in range(MATS):
        for copy in hops[m]:
            copy.wait_send()
    for copy in (*id_copies, *c1_copies, *c2_copies, *m1_copies, *m2_copies):
        copy.wait_send()

    def sent(i, carry):
        result_copy(i).wait_send()
        return carry

    lax.fori_loop(0, COLS - 1, sent, 0)


def final_kernel(st, total, pq, new_block, coefficients, factor, *, entries):
    inverse_root = 1.0 / math.sqrt(entries)
    tot = total[...]
    raw = tot * inverse_root
    both = jnp.dot(raw[:, 0:KP], pq[...], precision=lax.Precision.HIGHEST, preferred_element_type=F32)
    coefficients[...] = both[:, 0:KD]

    sub = lax.broadcasted_iota(jnp.int32, (BS, TILE), 0)
    lane = lax.broadcasted_iota(jnp.int32, (BS, TILE), 1)
    basis_part = lane < KP
    turned = jnp.where(basis_part, pltpu.roll(both, TILE // 2, 1), 0.0)

    def parts_of(index):
        return (lane == index + KP) | (lane == index + KP + 8) | (lane == index + KP + 16)

    def spread(value, j):
        return jnp.broadcast_to(value[j : j + 1, :], (BS, TILE))

    columns = [
        jnp.broadcast_to(
            jnp.sum(jnp.where(parts_of(j), tot, 0.0) - turned * spread(raw, j), axis=1, keepdims=True)
            * (1.0 / entries),
            (BS, TILE),
        )
        for j in range(BS)
    ]
    target = jnp.where(basis_part, both * -inverse_root, 0.0) + jnp.where(parts_of(sub), 1.0, 0.0)
    lower = jnp.zeros((BS, TILE), F32)
    for j in range(BS):
        pivot = spread(columns[j], j)
        scale = lax.rsqrt(pivot)
        scale = scale * (1.5 - 0.5 * pivot * scale * scale)
        column = columns[j] * scale
        below = jnp.where(sub > j, column, 0.0)
        lower = jnp.where((lane == j) & (sub >= j), column, lower)
        solved = spread(target, j) * scale
        target = jnp.where(sub == j, solved, target - below * solved)
        for i in range(j + 1, BS):
            columns[i] = columns[i] - below * spread(below, i)
    factor[...] = lower[:, 0:BS]
    mix = jnp.concatenate(split3(target[:, 0:STACK]), axis=0).astype(BF16)
    length = st.shape[1]
    for n in range(length // 512):
        part = slice(n * 512, (n + 1) * 512)
        wide = jnp.dot(mix, st[:, part], preferred_element_type=F32)
        new_block[:, part] = (wide[16:24] + wide[8:16]) + wide[0:8]


def shards(basis, expand, tiles, tile_rows, tile_cols):
    length = basis.shape[1]
    vmem = pl.BlockSpec(memory_space=pltpu.VMEM)
    hbm = pl.BlockSpec(memory_space=pltpu.HBM)
    dma = pltpu.SemaphoreType.DMA
    st, total, pq = pl.pallas_call(
        step_kernel,
        out_shape=(
            jax.ShapeDtypeStruct((STACK, length), BF16),
            jax.ShapeDtypeStruct((BS, TILE), F32),
            jax.ShapeDtypeStruct((KP, TILE), F32),
        ),
        in_specs=[hbm] * 5,
        out_specs=(vmem, vmem, vmem),
        scratch_shapes=[
            pltpu.VMEM(basis.shape, BF16),
            pltpu.VMEM(expand.shape, F32),
            pltpu.SMEM(tile_rows.shape, jnp.int32),
            pltpu.SMEM(tile_cols.shape, jnp.int32),
            pltpu.VMEM(tiles.shape, BF16),
            pltpu.VMEM((ROWS, MATS, 256, TILE), BF16),
            pltpu.VMEM((MATS, ROWS * REGION, BS, TILE), F32),
            pltpu.VMEM((COLS, PER * BS, TILE), F32),
            pltpu.VMEM((COLS, PER * BS, TILE), BF16),
            pltpu.VMEM((COLS, PER * BS, TILE), BF16),
            pltpu.VMEM((COLS, SLOTS * BS, TILE), F32),
            pltpu.VMEM((REGION * BS, TILE), F32),
            pltpu.VMEM((REGION, COLS * SLOTS), BF16),
            pltpu.VMEM((COLS, SLOTS, TILE), jnp.int32),
            pltpu.VMEM((COLS, SLOTS, TILE), jnp.int32),
            pltpu.VMEM((COLS, 16, TILE), F32),
            pltpu.VMEM((ROWS, 16, TILE), F32),
            pltpu.VMEM((COLS, BS, TILE), F32),
            pltpu.VMEM((ROWS, BS, TILE), F32),
            pltpu.VMEM((KP, TILE), F32),
            dma((4,)),
            dma((MATS, 3)),
            dma((MATS, 9)), dma((MATS, 9)),
            dma((COLS,)), dma((COLS,)),
            dma((COLS,)), dma((COLS,)),
            dma((ROWS,)), dma((ROWS,)),
            dma((COLS,)), dma((COLS,)),
            dma((COLS,)), dma((COLS,)),
            dma((ROWS,)), dma((ROWS,)),
        ],
        compiler_params=pltpu.CompilerParams(
            collective_id=0, has_side_effects=True, vmem_limit_bytes=36 * 2**20
        ),
        name="toar_step",
    )(*(pltpu.with_memory_space_constraint(a, pltpu.HBM) for a in (basis, expand, tile_rows, tile_cols, tiles)))
    return tuple(
        pl.pallas_call(
            functools.partial(final_kernel, entries=length * ROWS * COLS),
            out_shape=(
                jax.ShapeDtypeStruct((BS, length), F32),
                jax.ShapeDtypeStruct((BS, KD), F32),
                jax.ShapeDtypeStruct((BS, BS), F32),
            ),
            in_specs=[vmem, vmem, vmem],
            out_specs=(vmem, vmem, vmem),
            compiler_params=pltpu.CompilerParams(vmem_limit_bytes=8 * 2**20),
            name="toar_final",
        )(st, total, pq)
    )


def solution(mesh):
    finer = Mesh(mesh.devices.reshape(SIZES), AXES)
    return jax.shard_map(
        shards,
        mesh=finer,
        in_specs=(P(None, AXES), P(), P(None, AXES, None, None), P(AXES), P(AXES)),
        out_specs=(P(None, AXES), P(), P()),
        check_vma=False,
    )
```
